128 devices in a mesh: elem: 128 (over z, y, x, core).
Axes of the slice: x: 4, y: 4, z: 4, core: 2. Of those that a mesh axis runs over, the one named last changes fastest.
Arguments:
- tracers: float32 [2048, 4, 16, 128], P('elem'), may hold values from -6 to 6
- sources: float32 [2048, 4, 16, 128], P('elem'), may hold values from -3 to 3
- weights: float32 [2048, 4, 256], P('elem'), may hold values from -0.3 to 0.425
- dep_owner: int32 [2048, 4, 16], P('elem'), may hold values from 0 to 127, as said below
- dep_slot: int32 [2048, 4, 16], P('elem'), may hold values from 0 to 15, as said below
- nbr_elem: int32 [2048, 4], P('elem'), may hold values from 0 to 2047, as said below
- nbr_edge: int32 [2048, 4], P('elem'), may hold values from 0 to 3, as said below
- metric: float32 [2048, 2, 16], P('elem'), may hold values from 0.5 to 2
Outputs:
- settled: float32 [2048, 4, 16, 128], P('elem')
The draws below stay inside these ranges and needn't reach their ends.
Inputs may be any that keep to these rules, and one draw needn't show every extreme that they name: `dep_owner`: the departure element of a target point is its own element or one of its four edge neighbours, so its owner is the point's own device or the one before or after it, cyclically. Of one device's target points at most 1024 have departure elements on the next device and at most 1024 on the previous one; each bound is reached on some device in every draw. `dep_slot`: together with dep_owner it names the departure element. `nbr_elem`: global index is owner times 16 plus position. Edges are listed counterclockwise; the relation is symmetric and no element is its own neighbour. Every neighbour lies on the same device or the one before or after it, cyclically; exactly 16 edges of one device's elements face the next device and exactly 16 the previous one. `nbr_edge`: the neighbour's entry for that edge points back to the element and edge.
All inputs are finite; a program needn't handle non-finite values.
Results may differ from the reference program's by a relative error of at most 0.0003.
Values sent between devices are 32-bit elements; how exact they have to be, the bound alone decides.
A program may use at most 128 MiB of HBM per device.

```python
import math
import jax
import jax.numpy as jnp
import numpy as np
from jax import lax

GLL = 16
Q = 128
LEV = 4
BX = 16
EL_DEV = 16
ELEMS = 2048


def element_mesh(key):
    base = jax.random.fold_in(key, 7)
    devices = ELEMS // EL_DEV
    rows_each = EL_DEV // BX
    total_rows = devices * rows_each
    device_keys = jax.random.split(jax.random.fold_in(base, 1), devices)
    layout = jax.vmap(lambda sub_key: jax.random.permutation(sub_key, EL_DEV))(device_keys).astype(jnp.int32)
    inverse = jnp.argsort(layout, axis=1).astype(jnp.int32)
    rotation = jax.random.randint(jax.random.fold_in(base, 2), (ELEMS,), 0, 4, dtype=jnp.int32)
    owner_dev = jnp.arange(ELEMS, dtype=jnp.int32) // EL_DEV
    grid_cell = layout.reshape(-1)
    grid_row = owner_dev * rows_each + grid_cell // BX
    grid_col = grid_cell % BX
    row_step = jnp.array([-1, 0, 1, 0], jnp.int32)
    col_step = jnp.array([0, 1, 0, -1], jnp.int32)
    new_row = (grid_row[:, None] + row_step[None, :]) % total_rows
    new_col = (grid_col[:, None] + col_step[None, :]) % BX
    new_owner = new_row // rows_each
    new_cell = new_row % rows_each * BX + new_col
    by_direction = new_owner * EL_DEV + inverse[new_owner, new_cell]
    return (by_direction, rotation)


def neighbour_lists(key):
    by_direction, rotation = element_mesh(key)
    sides = jnp.arange(4, dtype=jnp.int32)
    direction = (sides[None, :] + rotation[:, None]) % 4
    across = jnp.take_along_axis(by_direction, direction, axis=1)
    back_dir = (direction + 2) % 4
    their_edge = (back_dir - rotation[across]) % 4
    return (across.astype(jnp.int32), their_edge.astype(jnp.int32))


def departures(key):
    by_direction, rotation = element_mesh(key)
    devices = ELEMS // EL_DEV
    base = jax.random.fold_in(key, 19)
    upward = jax.random.randint(jax.random.fold_in(base, 1), (devices,), 1, 11, dtype=jnp.int32)
    downward = jax.random.randint(jax.random.fold_in(base, 2), (devices,), 1, 11, dtype=jnp.int32)
    forced_up = jax.random.randint(jax.random.fold_in(base, 3), (), 0, devices, dtype=jnp.int32)
    forced_down = (forced_up + 1 + jax.random.randint(jax.random.fold_in(base, 4), (), 0, devices - 1, dtype=jnp.int32)) % devices
    device_ids = jnp.arange(devices, dtype=jnp.int32)
    upward = jnp.where(device_ids == forced_up, 20, jnp.where(device_ids == forced_down, 0, upward))
    downward = jnp.where(device_ids == forced_down, 20, jnp.where(device_ids == forced_up, 0, downward))
    throws = jax.random.randint(jax.random.fold_in(base, 5), (ELEMS, LEV, GLL), 0, 20, dtype=jnp.int32)
    owner_dev = jnp.arange(ELEMS, dtype=jnp.int32) // EL_DEV
    up_share = upward[owner_dev][:, None, None]
    down_share = downward[owner_dev][:, None, None]
    remainder = throws % 3
    grid_dir = jnp.where(throws < up_share, 2, jnp.where(throws < up_share + down_share, 0, jnp.where(remainder == 0, -1, jnp.where(remainder == 1, 1, 3))))
    self_ids = jnp.broadcast_to(jnp.arange(ELEMS, dtype=jnp.int32)[:, None, None], (ELEMS, LEV, GLL))
    chosen = jnp.where(grid_dir < 0, self_ids, by_direction[self_ids, jnp.maximum(grid_dir, 0)])
    return ((chosen // EL_DEV).astype(jnp.int32), (chosen % EL_DEV).astype(jnp.int32))


def draw_dep_owner(key, part):
    return departures(key)[0]


def draw_dep_slot(key, part):
    return departures(key)[1]


def draw_nbr_elem(key, part):
    return neighbour_lists(key)[0]


def draw_nbr_edge(key, part):
    return neighbour_lists(key)[1]


def level_of(stream_key, extent, cuts, smallest, high):
    gain = 1.0
    for position, parts in cuts:
        heights = jax.random.uniform(jax.random.fold_in(jax.random.fold_in(stream_key, 6), position), (parts,), jnp.float32, smallest / len(cuts), high / len(cuts))
        gain = gain * jnp.repeat(jnp.exp(heights), extent[position] // parts).reshape((-1,) + (1,) * (len(extent) - 1 - position))
    return gain


def centred(stream_key, shape, width, bound, pieces=(), held_as=jnp.bfloat16):
    level = level_of(stream_key, shape, pieces, -0.22, 0.18) if pieces else 1.0
    drawn = jax.random.normal(stream_key, shape, jnp.float32) * width * level
    return jnp.minimum(jnp.maximum(drawn, -bound), bound).astype(held_as)


def setup_inputs(seed: int = 0) -> dict:
    key_of = jax.random.split(jax.random.key(seed), 9)
    tracers = centred(key_of[0], (ELEMS, LEV, GLL, Q), 1.0, 6.0, ((0, 128),), jnp.float32)
    sources = centred(key_of[1], (ELEMS, LEV, GLL, Q), 0.5, 3.0, ((0, 128),), jnp.float32)
    weights = jnp.clip(-0.3 + 0.725 * jax.random.uniform(key_of[2], (ELEMS, LEV, GLL * GLL), jnp.float32) ** level_of(key_of[2], (ELEMS, LEV, GLL * GLL), ((0, 128),), -0.2, 0.2), -0.3, 0.425)
    dep_owner = draw_dep_owner(jax.random.fold_in(key_of[8], 71), 0)
    dep_slot = draw_dep_slot(jax.random.fold_in(key_of[8], 71), 0)
    nbr_elem = draw_nbr_elem(jax.random.fold_in(key_of[8], 71), 0)
    nbr_edge = draw_nbr_edge(jax.random.fold_in(key_of[8], 71), 0)
    metric = jnp.clip(jnp.exp(math.log(2.0) - 1.3862944 * jax.random.uniform(key_of[7], (ELEMS, 2, GLL), jnp.float32) ** level_of(key_of[7], (ELEMS, 2, GLL), ((0, 128),), -0.2, 0.2)), 0.5, 2.0)
    return dict(tracers=tracers, sources=sources, weights=weights, dep_owner=dep_owner, dep_slot=dep_slot, nbr_elem=nbr_elem, nbr_edge=nbr_edge, metric=metric)


VISCOSITY = 0.002
HIGH = lax.Precision.HIGHEST

def gll_tables():
    gll_nodes = np.array([-1.0, -np.sqrt(0.2), np.sqrt(0.2), 1.0])
    node_count = gll_nodes.shape[0]
    bary_weights = np.array([1.0 / np.prod([gll_nodes[j] - gll_nodes[m] for m in range(node_count) if m != j]) for j in range(node_count)])
    derivative = np.zeros((node_count, node_count))
    for i in range(node_count):
        for j in range(node_count):
            if i != j:
                derivative[i, j] = bary_weights[j] / bary_weights[i] / (gll_nodes[i] - gll_nodes[j])
        derivative[i, i] = -np.sum(derivative[i])
    identity = np.eye(node_count)
    along_a = np.kron(derivative, identity)
    along_b = np.kron(identity, derivative)
    edge_points = np.array([[4 * k for k in range(4)], [12 + k for k in range(4)], [4 * (3 - k) + 3 for k in range(4)], [3 - k for k in range(4)]], dtype=np.int32)
    spread = np.zeros((4, 4, 16))
    for s in range(4):
        for k in range(4):
            spread[s, k, edge_points[s, k]] = 1.0
    counts = 1.0 + spread.sum(axis=(0, 1))
    return (along_a, along_b, edge_points, spread, counts)

def interpolate(source_table, rows_from, block_weights):
    level_count = rows_from.shape[1]
    points = rows_from.shape[2]
    shaped = block_weights.reshape(block_weights.shape[0], level_count, points, points)
    levels_out = []
    for level in range(level_count):
        gathered = source_table[rows_from[:, level], level]
        levels_out.append(lax.optimization_barrier(jnp.sum(shaped[:, level][..., None] * gathered, axis=2)))
    return jnp.stack(levels_out, axis=1)

def local_laplacian(field_in, metric, tables):
    along_a = jnp.asarray(tables[0], field_in.dtype)
    along_b = jnp.asarray(tables[1], field_in.dtype)
    grad_a = jnp.einsum('pm,elmq->elpq', along_a, field_in, precision=HIGH)
    grad_b = jnp.einsum('pm,elmq->elpq', along_b, field_in, precision=HIGH)
    flux_a = metric[:, 0][:, None, :, None] * grad_a
    flux_b = metric[:, 1][:, None, :, None] * grad_b
    return jnp.einsum('pm,elmq->elpq', along_a, flux_a, precision=HIGH) + jnp.einsum('pm,elmq->elpq', along_b, flux_b, precision=HIGH)

def partner_edges(gathered, facing_edge, tables):
    reversed_points = jnp.asarray(tables[2][:, ::-1].copy(), jnp.int32)
    pick = (facing_edge[..., None] == jnp.arange(4, dtype=jnp.int32)).astype(jnp.int32)
    wanted = lax.optimization_barrier(jnp.sum(pick[..., None] * reversed_points, axis=2))
    select = (wanted[..., None] == jnp.arange(gathered.shape[3], dtype=jnp.int32)).astype(gathered.dtype)
    return jnp.einsum('eskp,eslpq->eslkq', select, gathered, precision=HIGH)

def close_edges(field_in, received, tables):
    spread = jnp.asarray(tables[3], field_in.dtype)
    counts = jnp.asarray(tables[4], field_in.dtype)
    added = jnp.einsum('skp,eslkq->elpq', spread, received, precision=HIGH)
    return (field_in + added) / counts[None, None, :, None]

def advect(field_in, dep_owner, dep_slot, weights):
    where_from = dep_owner * EL_DEV + dep_slot
    blocks = field_in.shape[0] // EL_DEV

    def one_block(block):
        start = block * EL_DEV
        rows_from = lax.dynamic_slice_in_dim(where_from, start, EL_DEV, 0)
        block_weights = lax.dynamic_slice_in_dim(weights, start, EL_DEV, 0)
        return interpolate(field_in, rows_from, block_weights)
    return lax.map(one_block, jnp.arange(blocks, dtype=jnp.int32)).reshape(field_in.shape)

def edge_close(field_in, nbr_elem, nbr_edge, tables):
    blocks = field_in.shape[0] // EL_DEV

    def one_block(block):
        start = block * EL_DEV
        own_values = lax.dynamic_slice_in_dim(field_in, start, EL_DEV, 0)
        partner = lax.dynamic_slice_in_dim(nbr_elem, start, EL_DEV, 0)
        facing = lax.dynamic_slice_in_dim(nbr_edge, start, EL_DEV, 0)
        received = partner_edges(field_in[partner], facing, tables)
        return close_edges(own_values, received, tables)
    return lax.map(one_block, jnp.arange(blocks, dtype=jnp.int32)).reshape(field_in.shape)

def reference(tracers, sources, weights, dep_owner, dep_slot, nbr_elem, nbr_edge, metric):
    tables = gll_tables()
    first = advect(tracers, dep_owner, dep_slot, weights) + sources
    second = advect(first, dep_owner, dep_slot, weights) + sources
    lap_once = edge_close(local_laplacian(second, metric, tables), nbr_elem, nbr_edge, tables)
    lap_twice = edge_close(local_laplacian(lap_once, metric, tables), nbr_elem, nbr_edge, tables)
    return second - VISCOSITY * lap_twice
```

```python
import functools

import jax
import jax.numpy as jnp
import numpy as np
from jax import lax
from jax.experimental import pallas as pl
from jax.experimental.pallas import tpu as pltpu
from jax.sharding import PartitionSpec as P

VISCOSITY = 0.002
HIGH = lax.Precision.HIGHEST
LEV = 4
PTS = 256
Q = 128
F32 = jnp.float32
BF16 = jnp.bfloat16
I32 = jnp.int32


def derivative_matrix():
    nodes = np.array([-1.0, -np.sqrt(0.2), np.sqrt(0.2), 1.0])
    count = nodes.shape[0]
    bary = np.array(
        [1.0 / np.prod([nodes[j] - nodes[m] for m in range(count) if m != j]) for j in range(count)]
    )
    derivative = np.zeros((count, count))
    for i in range(count):
        for j in range(count):
            if i != j:
                derivative[i, j] = bary[j] / bary[i] / (nodes[i] - nodes[j])
        derivative[i, i] = -np.sum(derivative[i])
    return derivative


def rows(shape):
    return lax.broadcasted_iota(I32, shape, 0)


def cols(shape):
    return lax.broadcasted_iota(I32, shape, 1)


def dot(a, b):
    return jnp.dot(a, b, preferred_element_type=F32)


def dot_exact(a, b):
    return jnp.dot(a, b, preferred_element_type=F32, precision=HIGH)


def split(x):
    hi = x.astype(BF16)
    lo = (x - hi.astype(F32)).astype(BF16)
    return hi, lo


def dot3(a_hi, a_lo, b_hi, b_lo):
    return dot(a_hi, b_hi) + (dot(a_hi, b_lo) + dot(a_lo, b_hi))


def edge_point(s, k):
    return jnp.where(s == 0, 4 * k, jnp.where(s == 1, 12 + k, jnp.where(s == 2, 15 - 4 * k, 3 - k)))


def direction_table(shape, along_b):
    m, p = rows(shape) & 15, cols(shape) & 15
    if along_b:
        i, j, live = m & 3, p & 3, (m >> 2) == (p >> 2)
    else:
        i, j, live = m >> 2, p >> 2, (m & 3) == (p & 3)
    which = jnp.where(live, i * 4 + j, -1)
    table = derivative_matrix()
    value = jnp.zeros(shape, F32)
    for at in range(16):
        value = jnp.where(which == at, np.float32(table[at // 4, at % 4]), value)
    return value


def offset_of(owner, me, count):
    d = owner - me
    d = jnp.where(d > 1, d - count, d)
    d = jnp.where(d < -1, d + count, d)
    return d + 1


def kernel(
    count,
    tracers, sources, weights, dep_owner, dep_slot, nbr_elem, nbr_edge, metric,
    out,
    own_t, src, wts, dow, dsl, nel, ned, met,
    f1, first, f2, second, part, outbuf,
    w_hi, w_lo,
    v_out, v_in, s3, x3,
    h_hi, h_lo, sm_hi, sm_lo, e_hi, e_lo,
    loc, loc_t, loc_o,
    send1, recv1, send2, recv2, send3, recv3, sendv, recvv,
):
    me = lax.axis_index("elem")

    def at(step):
        return lax.rem(me + step + count, count)

    small = [
        pltpu.make_async_copy(a, b, loc.at[i])
        for i, (a, b) in enumerate(
            [
                (weights, wts),
                (dep_owner, dow),
                (dep_slot, dsl),
                (nbr_elem, nel),
                (nbr_edge, ned),
                (metric, met),
            ]
        )
    ]
    load_t = [pltpu.make_async_copy(tracers.at[:, k], own_t.at[k], loc_t.at[0, k]) for k in range(LEV)]
    load_s = [pltpu.make_async_copy(sources.at[:, k], src.at[k], loc_t.at[1, k]) for k in range(LEV)]

    def remote(source, target, send_sem, recv_sem, step):
        return pltpu.make_async_remote_copy(
            src_ref=source,
            dst_ref=target,
            send_sem=send_sem,
            recv_sem=recv_sem,
            device_id=(at(step),),
            device_id_type=pl.DeviceIdType.MESH,
        )

    ex1 = [
        [remote(own_t.at[k], f1.at[k, i], send1.at[k, i], recv1.at[k, i], (1, -1)[i]) for i in range(2)]
        for k in range(LEV)
    ]
    ex2 = [
        [remote(first.at[k], f2.at[k, i], send2.at[k, i], recv2.at[k, i], (1, -1)[i]) for i in range(2)]
        for k in range(LEV)
    ]
    exv = [
        remote(v_out.at[pl.ds(64 * i, 64)], v_in.at[i], sendv.at[i], recvv.at[i], (1, -1)[i])
        for i in range(2)
    ]
    spans = [(0, 128, 0, 1), (128, 128, 128, -1), (0, 64, 256, 2), (128, 64, 320, -2)]
    ex3 = [
        [
            remote(
                s3.at[k, pl.ds(a, size)], x3.at[k, pl.ds(b, size)], send3.at[k, i], recv3.at[k, i], step
            )
            for i, (a, size, b, step) in enumerate(spans)
        ]
        for k in range(LEV)
    ]

    barrier = pltpu.get_barrier_semaphore()
    for step in (1, -1, 2, -2):
        pl.semaphore_signal(
            barrier, inc=1, device_id=(at(step),), device_id_type=pl.DeviceIdType.MESH
        )
    for c in load_t:
        c.start()
    for c in small:
        c.start()
    for c in load_s:
        c.start()
    for c in load_t:
        c.wait()
    pl.semaphore_wait(barrier, 4)
    for k in range(LEV):
        for c in ex1[k]:
            c.start()

    for c in small:
        c.wait()
    for c in load_s:
        c.wait()
    diagonal = (cols((16, PTS)) >> 4) == rows((16, PTS))
    eye16 = cols((16, 16)) == rows((16, 16))
    tile_j = ((rows((PTS, PTS)) & 15) == (cols((PTS, PTS)) & 15)).astype(F32).astype(BF16)
    lane_elem = (cols((1, PTS)) >> 4).astype(F32)

    def advection_matrix(k):
        his, los, codes = [], [], []
        for e in range(16):
            row = wts[e, pl.ds(k, 1), :]
            hi = row.astype(BF16).astype(F32)
            his.append(jnp.where(diagonal, jnp.broadcast_to(hi, (16, PTS)), 0.0))
            los.append(jnp.where(diagonal, jnp.broadcast_to(row - hi, (16, PTS)), 0.0))
            code = offset_of(dow[e, pl.ds(k, 1), :], me, count) * 16 + dsl[e, pl.ds(k, 1), :]
            codes.append(jnp.where(eye16, jnp.broadcast_to(code.astype(F32), (16, 16)), 0.0))
        hi = dot(jnp.concatenate(his, axis=0).astype(BF16), tile_j)
        lo = dot(jnp.concatenate(los, axis=0).astype(BF16), tile_j)
        code = jnp.sum(jnp.concatenate(codes, axis=0), axis=1, keepdims=True)
        for i in range(3):
            match = code == (lane_elem + float(16 * i))
            w_hi[k, i] = jnp.where(match, hi, 0.0).astype(BF16)
            w_lo[k, i] = jnp.where(match, lo, 0.0).astype(BF16)

    def mix(k, i, field):
        hi, lo = split(field.reshape(PTS, Q))
        return dot3(w_hi[k, i], w_lo[k, i], hi, lo)

    def cube(x):
        return x.reshape(16, 16, Q)

    for k in range(LEV):
        advection_matrix(k)
        first[k] = cube(mix(k, 1, own_t[k])) + src[k]

    square = (PTS, PTS)
    r, c = rows(square), cols(square)
    same_elem = (r >> 4) == (c >> 4)
    unit = r == c
    left_a, left_b = direction_table((16, 16), False), direction_table((16, 16), True)
    right_a, right_b = direction_table((16, PTS), False), direction_table((16, PTS), True)
    fa, fb, ne_rows, nt_rows = [], [], [], []
    pick = (rows((16, 4)) >> 2) == cols((16, 4))
    for e in range(16):
        fa.append(left_a * jnp.broadcast_to(met[e, pl.ds(0, 1), :], (16, 16)))
        fb.append(left_b * jnp.broadcast_to(met[e, pl.ds(1, 1), :], (16, 16)))
        ne_rows.append(jnp.where(pick, jnp.broadcast_to(nel[pl.ds(e, 1), :], (16, 4)), 0).astype(F32))
        nt_rows.append(jnp.where(pick, jnp.broadcast_to(ned[pl.ds(e, 1), :], (16, 4)), 0).astype(F32))
    full = dot_exact(jnp.concatenate(fa, axis=0), right_a) + dot_exact(jnp.concatenate(fb, axis=0), right_b)
    m = jnp.where(same_elem, full, 0.0)

    ne = jnp.sum(jnp.concatenate(ne_rows, axis=0), axis=1, keepdims=True).astype(I32)
    nt = jnp.sum(jnp.concatenate(nt_rows, axis=0), axis=1, keepdims=True).astype(I32)
    off = offset_of(ne >> 4, me, count)
    pe = (ne & 15) * 4 + nt
    off_f, pe_f = off.astype(F32), pe.astype(F32)
    off_row = jnp.sum(jnp.where(unit, off_f, 0.0), axis=0, keepdims=True)
    pe_row = jnp.sum(jnp.where(unit, pe_f, 0.0), axis=0, keepdims=True)
    peer = (off_row == off_f) & ((c & 3) == 0)
    rank_own = jnp.sum(jnp.where(peer & ((c >> 2) < (r >> 2)), 1.0, 0.0), axis=1, keepdims=True).astype(I32)
    rank_pe = jnp.sum(jnp.where(peer & (pe_row < pe_f), 1.0, 0.0), axis=1, keepdims=True).astype(I32)
    point = rows((PTS, 1)) & 3
    slot = jnp.where(off == 1, pe, jnp.where(off == 0, 64 + rank_pe, 80 + rank_pe))
    take = (cols((PTS, 384)) == slot * 4 + 3 - point).astype(F32).astype(BF16)
    place = jnp.where(off == 1, -1, jnp.where(off == 2, 0, 64) + rank_own * 4 + point)
    pack_t = (cols((PTS, 128)) == place).astype(F32)
    pack = pack_t.T.astype(BF16)
    spread_t = (same_elem & ((r & 15) == edge_point((c >> 2) & 3, c & 3))).astype(F32).astype(BF16)
    spread = (same_elem & ((c & 15) == edge_point((r >> 2) & 3, r & 3))).astype(F32).astype(BF16)
    a, b = (rows((PTS, 1)) >> 2) & 3, rows((PTS, 1)) & 3
    rim_a, rim_b = ((a == 0) | (a == 3)).astype(F32), ((b == 0) | (b == 3)).astype(F32)
    counts = 1.0 + rim_a + rim_b
    added = dot(spread_t, take)
    own_add = dot(added[:, :PTS].astype(BF16), spread)
    r_own = (jnp.where(unit, 1.0, 0.0) + own_add) / counts
    r_out = added[:, PTS:] / counts
    picked = dot(pack, spread)
    km = dot_exact(picked, m)
    g = dot_exact(r_own, m)
    v = dot_exact(km, r_out)
    v_out[...] = v
    for cpy in exv:
        cpy.start()
    kmg = dot_exact(km, g)
    sm = jnp.concatenate([km[:64], kmg[:64], km[64:], kmg[64:]], axis=0)
    hi, lo = split(sm)
    sm_hi[...] = hi
    sm_lo[...] = lo
    gr = dot_exact(g, r_out)
    gg = dot_exact(g, g)

    for k in range(LEV):
        total = first[k].reshape(PTS, Q)
        for i in range(2):
            ex1[k][i].wait_recv()
            total = total + mix(k, 2 * i, f1[k, i])
        first[k] = cube(total)
        for cpy in ex2[k]:
            cpy.start()
        part[k] = mix(k, 1, total) + src[k].reshape(PTS, Q)

    for cpy in exv:
        cpy.wait_recv()
    from_prev, from_next = v_in[0], v_in[1]
    rv_p = dot_exact(r_out[:, :64], from_prev)
    rv_n = dot_exact(r_out[:, 64:], from_next)
    twice = gg + dot_exact(rv_p[:, 64:], km[64:]) + dot_exact(rv_n[:, :64], km[:64])
    h = jnp.where(unit, 1.0, 0.0) - VISCOSITY * twice
    hi, lo = split(h)
    h_hi[...] = hi
    h_lo[...] = lo
    ext = -VISCOSITY * jnp.concatenate(
        [gr[:, :64], r_out[:, :64], gr[:, 64:], r_out[:, 64:], rv_p[:, :64], rv_n[:, 64:]], axis=1
    )
    hi, lo = split(ext)
    e_hi[...] = hi
    e_lo[...] = lo

    for k in range(LEV):
        total = part[k]
        for i in range(2):
            ex2[k][i].wait_recv()
            total = total + mix(k, 2 * i, f2[k, i])
        hi, lo = split(total)
        s3[k] = dot3(sm_hi[...], sm_lo[...], hi, lo)
        for cpy in ex3[k]:
            cpy.start()
        part[k] = dot3(h_hi[...], h_lo[...], hi, lo)

    stores = []
    for k in range(LEV):
        for cpy in ex3[k]:
            cpy.wait_recv()
        hi, lo = split(x3[k])
        outbuf[k] = cube(part[k] + dot3(e_hi[...], e_lo[...], hi, lo))
        store = pltpu.make_async_copy(outbuf.at[k], out.at[:, k], loc_o.at[k])
        store.start()
        stores.append(store)
    for group in ex1 + ex2 + ex3 + [exv]:
        for cpy in group:
            cpy.wait_send()
    for store in stores:
        store.wait()


def local(tracers, sources, weights, dep_owner, dep_slot, nbr_elem, nbr_edge, metric):
    count = lax.axis_size("elem")
    block = (LEV, 16, 16, Q)
    dma = pltpu.SemaphoreType.DMA
    vmem = pltpu.VMEM
    scratch = [
        vmem(block, F32), vmem(block, F32), vmem(weights.shape, F32),
        vmem(dep_owner.shape, I32), vmem(dep_slot.shape, I32),
        vmem(nbr_elem.shape, I32), vmem(nbr_edge.shape, I32), vmem(metric.shape, F32),
        vmem((LEV, 2, 16, 16, Q), F32), vmem(block, F32), vmem((LEV, 2, 16, 16, Q), F32),
        vmem((8, 128), F32), vmem((LEV, PTS, Q), F32), vmem(block, F32),
        vmem((LEV, 3, PTS, PTS), BF16), vmem((LEV, 3, PTS, PTS), BF16),
        vmem((128, 128), F32), vmem((2, 64, 128), F32),
        vmem((LEV, PTS, Q), F32), vmem((LEV, 384, Q), F32),
        vmem((PTS, PTS), BF16), vmem((PTS, PTS), BF16),
        vmem((PTS, PTS), BF16), vmem((PTS, PTS), BF16),
        vmem((PTS, 384), BF16), vmem((PTS, 384), BF16),
        dma((6,)), dma((2, LEV)), dma((LEV,)),
        dma((LEV, 2)), dma((LEV, 2)), dma((LEV, 2)), dma((LEV, 2)),
        dma((LEV, 4)), dma((LEV, 4)), dma((2,)), dma((2,)),
    ]
    return pl.pallas_call(
        functools.partial(kernel, count),
        out_shape=jax.ShapeDtypeStruct(tracers.shape, F32),
        in_specs=[pl.BlockSpec(memory_space=pl.ANY)] * 8,
        out_specs=pl.BlockSpec(memory_space=pl.ANY),
        scratch_shapes=scratch,
        compiler_params=pltpu.CompilerParams(collective_id=0, has_side_effects=True),
        name="tracer_step",
    )(tracers, sources, weights, dep_owner, dep_slot, nbr_elem, nbr_edge, metric)


def solution(mesh):
    placed = (
        P("elem", None, None, None),
        P("elem", None, None, None),
        P("elem", None, None),
        P("elem", None, None),
        P("elem", None, None),
        P("elem", None),
        P("elem", None),
        P("elem", None, None),
    )
    return jax.shard_map(
        local, mesh=mesh, in_specs=placed, out_specs=P("elem", None, None, None), check_vma=False
    )
```

```python
import functools

import jax
import jax.numpy as jnp
import numpy as np
from jax import lax
from jax.experimental import pallas as pl
from jax.experimental.pallas import tpu as pltpu
from jax.sharding import PartitionSpec as P

VISCOSITY = 0.002
HIGH = lax.Precision.HIGHEST
LEV = 4
PTS = 256
Q = 128
F32 = jnp.float32
BF16 = jnp.bfloat16
I32 = jnp.int32


def derivative_matrix():
    nodes = np.array([-1.0, -np.sqrt(0.2), np.sqrt(0.2), 1.0])
    count = nodes.shape[0]
    bary = np.array(
        [1.0 / np.prod([nodes[j] - nodes[m] for m in range(count) if m != j]) for j in range(count)]
    )
    derivative = np.zeros((count, count))
    for i in range(count):
        for j in range(count):
            if i != j:
                derivative[i, j] = bary[j] / bary[i] / (nodes[i] - nodes[j])
        derivative[i, i] = -np.sum(derivative[i])
    return derivative


def rows(shape):
    return lax.broadcasted_iota(I32, shape, 0)


def cols(shape):
    return lax.broadcasted_iota(I32, shape, 1)


def dot(a, b):
    return jnp.dot(a, b, preferred_element_type=F32)


def dot_exact(a, b):
    return jnp.dot(a, b, preferred_element_type=F32, precision=HIGH)


def split(x):
    hi = x.astype(BF16)
    lo = (x - hi.astype(F32)).astype(BF16)
    return hi, lo


def dot3(a_hi, a_lo, b_hi, b_lo):
    return dot(a_hi, b_hi) + (dot(a_hi, b_lo) + dot(a_lo, b_hi))


def edge_point(s, k):
    return jnp.where(s == 0, 4 * k, jnp.where(s == 1, 12 + k, jnp.where(s == 2, 15 - 4 * k, 3 - k)))


def direction_table(shape, along_b):
    m, p = rows(shape) & 15, cols(shape) & 15
    if along_b:
        i, j, live = m & 3, p & 3, (m >> 2) == (p >> 2)
    else:
        i, j, live = m >> 2, p >> 2, (m & 3) == (p & 3)
    which = jnp.where(live, i * 4 + j, -1)
    table = derivative_matrix()
    value = jnp.zeros(shape, F32)
    for at in range(16):
        value = jnp.where(which == at, np.float32(table[at // 4, at % 4]), value)
    return value


def offset_of(owner, me, count):
    d = owner - me
    d = jnp.where(d > 1, d - count, d)
    d = jnp.where(d < -1, d + count, d)
    return d + 1


def kernel(
    count,
    tracers, sources, weights, dep_owner, dep_slot, nbr_elem, nbr_edge, metric,
    outbuf,
    own_t, src, wts, dow, dsl, nel, ned, met,
    f1, first, f2, part,
    w_hi, w_lo,
    v_out, v_in, s3, x3,
    h_hi, h_lo, sm_hi, sm_lo, e_hi, e_lo,
    loc, loc_t,
    send1, recv1, send2, recv2, send3, recv3, sendv, recvv,
):
    me = lax.axis_index("elem")

    def at(step):
        return lax.rem(me + step + count, count)

    small = [
        pltpu.make_async_copy(a, b, loc.at[i])
        for i, (a, b) in enumerate(
            [
                (weights, wts),
                (dep_owner, dow),
                (dep_slot, dsl),
                (nbr_elem, nel),
                (nbr_edge, ned),
                (metric, met),
            ]
        )
    ]
    load_t = [pltpu.make_async_copy(tracers.at[:, k], own_t.at[k], loc_t.at[0, k]) for k in range(LEV)]
    load_s = [pltpu.make_async_copy(sources.at[:, k], src.at[k], loc_t.at[1, k]) for k in range(LEV)]

    def remote(source, target, send_sem, recv_sem, step):
        return pltpu.make_async_remote_copy(
            src_ref=source,
            dst_ref=target,
            send_sem=send_sem,
            recv_sem=recv_sem,
            device_id=(at(step),),
            device_id_type=pl.DeviceIdType.MESH,
        )

    ex1 = [
        [remote(own_t.at[k], f1.at[k, i], send1.at[k, i], recv1.at[k, i], (1, -1)[i]) for i in range(2)]
        for k in range(LEV)
    ]
    ex2 = [
        [remote(first.at[k], f2.at[k, i], send2.at[k, i], recv2.at[k, i], (1, -1)[i]) for i in range(2)]
        for k in range(LEV)
    ]
    exv = [
        remote(v_out.at[pl.ds(64 * i, 64)], v_in.at[i], sendv.at[i], recvv.at[i], (1, -1)[i])
        for i in range(2)
    ]
    spans = [(0, 128, 0, 1), (128, 128, 128, -1), (0, 64, 256, 2), (128, 64, 320, -2)]
    ex3 = [
        [
            remote(
                s3.at[k, pl.ds(a, size)], x3.at[k, pl.ds(b, size)], send3.at[k, i], recv3.at[k, i], step
            )
            for i, (a, size, b, step) in enumerate(spans)
        ]
        for k in range(LEV)
    ]

    barrier = pltpu.get_barrier_semaphore()
    for step in (1, -1, 2, -2):
        pl.semaphore_signal(
            barrier, inc=1, device_id=(at(step),), device_id_type=pl.DeviceIdType.MESH
        )
    for c in load_t:
        c.start()
    for c in small:
        c.start()
    for c in load_s:
        c.start()
    for c in load_t:
        c.wait()
    pl.semaphore_wait(barrier, 4)
    for k in range(LEV):
        for c in ex1[k]:
            c.start()

    for c in small:
        c.wait()
    for c in load_s:
        c.wait()
    diagonal = (cols((16, PTS)) >> 4) == rows((16, PTS))
    eye16 = cols((16, 16)) == rows((16, 16))
    tile_j = ((rows((PTS, PTS)) & 15) == (cols((PTS, PTS)) & 15)).astype(F32).astype(BF16)
    lane_elem = (cols((1, PTS)) >> 4).astype(F32)

    def advection_matrix(k):
        his, los, codes = [], [], []
        for e in range(16):
            row = wts[e, pl.ds(k, 1), :]
            hi = row.astype(BF16).astype(F32)
            his.append(jnp.where(diagonal, jnp.broadcast_to(hi, (16, PTS)), 0.0))
            los.append(jnp.where(diagonal, jnp.broadcast_to(row - hi, (16, PTS)), 0.0))
            code = offset_of(dow[e, pl.ds(k, 1), :], me, count) * 16 + dsl[e, pl.ds(k, 1), :]
            codes.append(jnp.where(eye16, jnp.broadcast_to(code.astype(F32), (16, 16)), 0.0))
        hi = dot(jnp.concatenate(his, axis=0).astype(BF16), tile_j)
        lo = dot(jnp.concatenate(los, axis=0).astype(BF16), tile_j)
        code = jnp.sum(jnp.concatenate(codes, axis=0), axis=1, keepdims=True)
        for i in range(3):
            match = code == (lane_elem + float(16 * i))
            w_hi[k, i] = jnp.where(match, hi, 0.0).astype(BF16)
            w_lo[k, i] = jnp.where(match, lo, 0.0).astype(BF16)

    def mix(k, i, field):
        hi, lo = split(field.reshape(PTS, Q))
        return dot3(w_hi[k, i], w_lo[k, i], hi, lo)

    def cube(x):
        return x.reshape(16, 16, Q)

    for k in range(LEV):
        advection_matrix(k)
        first[k] = cube(mix(k, 1, own_t[k])) + src[k]

    square = (PTS, PTS)
    r, c = rows(square), cols(square)
    same_elem = (r >> 4) == (c >> 4)
    unit = r == c
    left_a, left_b = direction_table((16, 16), False), direction_table((16, 16), True)
    right_a, right_b = direction_table((16, PTS), False), direction_table((16, PTS), True)
    fa, fb = [], []
    for e in range(16):
        fa.append(left_a * jnp.broadcast_to(met[e, pl.ds(0, 1), :], (16, 16)))
        fb.append(left_b * jnp.broadcast_to(met[e, pl.ds(1, 1), :], (16, 16)))
    full = dot_exact(jnp.concatenate(fa, axis=0), right_a) + dot_exact(jnp.concatenate(fb, axis=0), right_b)
    m = jnp.where(same_elem, full, 0.0)

    edge_row, edge_col = rows((PTS, 16)), cols((PTS, 16))

    def edge_column(table):
        spread_out = jnp.zeros((PTS, 16), F32)
        for s in range(4):
            here = ((edge_row >> 4) == edge_col) & (((edge_row >> 2) & 3) == s)
            line = table[pl.ds(s, 1), :].astype(F32)
            spread_out = jnp.where(here, jnp.broadcast_to(line, (PTS, 16)), spread_out)
        return jnp.sum(spread_out, axis=1, keepdims=True).astype(I32)

    ne, nt = edge_column(nel), edge_column(ned)
    off = offset_of(ne >> 4, me, count)
    pe = (ne & 15) * 4 + nt
    off_f, pe_f = off.astype(F32), pe.astype(F32)
    off_row = jnp.sum(jnp.where(unit, off_f, 0.0), axis=0, keepdims=True)
    pe_row = jnp.sum(jnp.where(unit, pe_f, 0.0), axis=0, keepdims=True)
    peer = (off_row == off_f) & ((c & 3) == 0)
    rank_own = jnp.sum(jnp.where(peer & ((c >> 2) < (r >> 2)), 1.0, 0.0), axis=1, keepdims=True).astype(I32)
    rank_pe = jnp.sum(jnp.where(peer & (pe_row < pe_f), 1.0, 0.0), axis=1, keepdims=True).astype(I32)
    point = rows((PTS, 1)) & 3
    slot = jnp.where(off == 1, pe, jnp.where(off == 0, 64 + rank_pe, 80 + rank_pe))
    take = (cols((PTS, 384)) == slot * 4 + 3 - point).astype(F32).astype(BF16)
    place = jnp.where(off == 1, -1, jnp.where(off == 2, 0, 64) + rank_own * 4 + point)
    pack_t = (cols((PTS, 128)) == place).astype(F32)
    pack = pack_t.T.astype(BF16)
    spread_t = (same_elem & ((r & 15) == edge_point((c >> 2) & 3, c & 3))).astype(F32).astype(BF16)
    spread = (same_elem & ((c & 15) == edge_point((r >> 2) & 3, r & 3))).astype(F32).astype(BF16)
    a, b = (rows((PTS, 1)) >> 2) & 3, rows((PTS, 1)) & 3
    rim_a, rim_b = ((a == 0) | (a == 3)).astype(F32), ((b == 0) | (b == 3)).astype(F32)
    counts = 1.0 + rim_a + rim_b
    added = dot(spread_t, take)
    own_add = dot(added[:, :PTS].astype(BF16), spread)
    r_own = (jnp.where(unit, 1.0, 0.0) + own_add) / counts
    r_out = added[:, PTS:] / counts
    picked = dot(pack, spread)
    km = dot_exact(picked, m)
    g = dot_exact(r_own, m)
    v = dot_exact(km, r_out)
    v_out[...] = v
    for cpy in exv:
        cpy.start()
    kmg = dot_exact(km, g)
    sm = jnp.concatenate([km[:64], kmg[:64], km[64:], kmg[64:]], axis=0)
    hi, lo = split(sm)
    sm_hi[...] = hi
    sm_lo[...] = lo
    gr = dot_exact(g, r_out)
    gg = dot_exact(g, g)

    for k in range(LEV):
        total = first[k].reshape(PTS, Q)
        for i in range(2):
            ex1[k][i].wait_recv()
            total = total + mix(k, 2 * i, f1[k, i])
        first[k] = cube(total)
        for cpy in ex2[k]:
            cpy.start()
        part[k] = mix(k, 1, total) + src[k].reshape(PTS, Q)

    for cpy in exv:
        cpy.wait_recv()
    from_prev, from_next = v_in[0], v_in[1]
    rv_p = dot_exact(r_out[:, :64], from_prev)
    rv_n = dot_exact(r_out[:, 64:], from_next)
    twice = gg + dot_exact(rv_p[:, 64:], km[64:]) + dot_exact(rv_n[:, :64], km[:64])
    h = jnp.where(unit, 1.0, 0.0) - VISCOSITY * twice
    hi, lo = split(h)
    h_hi[...] = hi
    h_lo[...] = lo
    ext = -VISCOSITY * jnp.concatenate(
        [gr[:, :64], r_out[:, :64], gr[:, 64:], r_out[:, 64:], rv_p[:, :64], rv_n[:, 64:]], axis=1
    )
    hi, lo = split(ext)
    e_hi[...] = hi
    e_lo[...] = lo

    for k in range(LEV):
        total = part[k]
        for i in range(2):
            ex2[k][i].wait_recv()
            total = total + mix(k, 2 * i, f2[k, i])
        hi, lo = split(total)
        s3[k] = dot3(sm_hi[...], sm_lo[...], hi, lo)
        for cpy in ex3[k]:
            cpy.start()
        part[k] = dot3(h_hi[...], h_lo[...], hi, lo)

    for k in range(LEV):
        for cpy in ex3[k]:
            cpy.wait_recv()
        hi, lo = split(x3[k])
        outbuf[:, k] = cube(part[k] + dot3(e_hi[...], e_lo[...], hi, lo))
    for group in ex1 + ex2 + ex3 + [exv]:
        for cpy in group:
            cpy.wait_send()


def local(tracers, sources, weights, dep_owner, dep_slot, nbr_elem, nbr_edge, metric):
    count = lax.axis_size("elem")
    block = (LEV, 16, 16, Q)
    dma = pltpu.SemaphoreType.DMA
    vmem = pltpu.VMEM
    scratch = [
        vmem(block, F32), vmem(block, F32), vmem(weights.shape, F32),
        vmem(dep_owner.shape, I32), vmem(dep_slot.shape, I32),
        vmem(nbr_elem.shape[::-1], I32), vmem(nbr_edge.shape[::-1], I32), vmem(metric.shape, F32),
        vmem((LEV, 2, 16, 16, Q), F32), vmem(block, F32), vmem((LEV, 2, 16, 16, Q), F32),
        vmem((LEV, PTS, Q), F32),
        vmem((LEV, 3, PTS, PTS), BF16), vmem((LEV, 3, PTS, PTS), BF16),
        vmem((128, 128), F32), vmem((2, 64, 128), F32),
        vmem((LEV, PTS, Q), F32), vmem((LEV, 384, Q), F32),
        vmem((PTS, PTS), BF16), vmem((PTS, PTS), BF16),
        vmem((PTS, PTS), BF16), vmem((PTS, PTS), BF16),
        vmem((PTS, 384), BF16), vmem((PTS, 384), BF16),
        dma((6,)), dma((2, LEV)),
        dma((LEV, 2)), dma((LEV, 2)), dma((LEV, 2)), dma((LEV, 2)),
        dma((LEV, 4)), dma((LEV, 4)), dma((2,)), dma((2,)),
    ]
    return pl.pallas_call(
        functools.partial(kernel, count),
        out_shape=pltpu.VMEM(tracers.shape, F32),
        in_specs=[pl.BlockSpec(memory_space=pl.ANY)] * 8,
        out_specs=pl.BlockSpec(memory_space=pltpu.VMEM),
        scratch_shapes=scratch,
        compiler_params=pltpu.CompilerParams(collective_id=0, has_side_effects=True),
        name="tracer_step",
    )(tracers, sources, weights, dep_owner, dep_slot, nbr_elem.T, nbr_edge.T, metric)


def solution(mesh):
    placed = (
        P("elem", None, None, None),
        P("elem", None, None, None),
        P("elem", None, None),
        P("elem", None, None),
        P("elem", None, None),
        P("elem", None),
        P("elem", None),
        P("elem", None, None),
    )
    return jax.shard_map(
        local, mesh=mesh, in_specs=placed, out_specs=P("elem", None, None, None), check_vma=False
    )
```

```python
import functools

import jax
import jax.numpy as jnp
import numpy as np
from jax import lax
from jax.experimental import pallas as pl
from jax.experimental.pallas import tpu as pltpu
from jax.sharding import PartitionSpec as P

VISCOSITY = 0.002
LEV = 4
PTS = 256
Q = 128
F32 = jnp.float32
BF16 = jnp.bfloat16
I32 = jnp.int32


def derivative_matrix():
    nodes = np.array([-1.0, -np.sqrt(0.2), np.sqrt(0.2), 1.0])
    count = nodes.shape[0]
    bary = np.array(
        [1.0 / np.prod([nodes[j] - nodes[m] for m in range(count) if m != j]) for j in range(count)]
    )
    derivative = np.zeros((count, count))
    for i in range(count):
        for j in range(count):
            if i != j:
                derivative[i, j] = bary[j] / bary[i] / (nodes[i] - nodes[j])
        derivative[i, i] = -np.sum(derivative[i])
    return derivative


def rows(shape):
    return lax.broadcasted_iota(I32, shape, 0)


def cols(shape):
    return lax.broadcasted_iota(I32, shape, 1)


def dot(a, b):
    return jnp.dot(a, b, preferred_element_type=F32)


def split(x):
    hi = x.astype(BF16)
    lo = (x - hi.astype(F32)).astype(BF16)
    return hi, lo


def dot3(a_hi, a_lo, b_hi, b_lo):
    n = b_hi.shape[1]
    both = dot(a_hi, jnp.concatenate([b_hi, b_lo], axis=1))
    return both[:, :n] + (both[:, n:] + dot(a_lo, b_hi))


def dot_split(a, b):
    return dot3(*split(a), *split(b))


def edge_point(s, k):
    return jnp.where(s == 0, 4 * k, jnp.where(s == 1, 12 + k, jnp.where(s == 2, 15 - 4 * k, 3 - k)))


def direction_table(shape, along_b):
    m, p = rows(shape) & 15, cols(shape) & 15
    if along_b:
        i, j, live = m & 3, p & 3, (m >> 2) == (p >> 2)
    else:
        i, j, live = m >> 2, p >> 2, (m & 3) == (p & 3)
    which = jnp.where(live, i * 4 + j, -1)
    table = derivative_matrix()
    value = jnp.zeros(shape, F32)
    for at in range(16):
        value = jnp.where(which == at, np.float32(table[at // 4, at % 4]), value)
    return value


def offset_of(owner, me, count):
    d = owner - me
    d = jnp.where(d > 1, d - count, d)
    d = jnp.where(d < -1, d + count, d)
    return d + 1


def kernel(
    count,
    tracers, sources, weights, dep_owner, dep_slot, nbr_elem, nbr_edge, metric,
    outbuf,
    own_t, src, wx, dow, dsl, nel, ned, met,
    f1, first, f2, base, total,
    w_hi, w_lo, wx_in, nb_hi, nb_lo,
    v_out, v_in, sm, sm_hi, sm_lo, sm_in, sn_hi, sn_lo,
    corr, vz_hi, vz_lo, once, twice_own, twice, once_in, twice_in, terms_in,
    h_hi, h_lo, e_hi, e_lo,
    loc, loc_t,
    send1, recv1, send2, recv2, sendm, recvm, sendp, recvp, sendq, recvq,
):
    me = lax.axis_index("elem")
    place_in_row = lax.rem(me, 8)
    near = jnp.where(place_in_row < 4, 1, 0)
    far = 1 - near
    edge = (place_in_row == 0) | (place_in_row == 7)
    middle = (place_in_row == 3) | (place_in_row == 4)

    def beyond(side):
        return lax.rem(me + 1 - 2 * side + count, count)

    def remote(source, target, send_sem, recv_sem, side):
        return pltpu.make_async_remote_copy(
            src_ref=source,
            dst_ref=target,
            send_sem=send_sem,
            recv_sem=recv_sem,
            device_id=(beyond(side),),
            device_id_type=pl.DeviceIdType.MESH,
        )

    small = [
        pltpu.make_async_copy(a, b, loc.at[i])
        for i, (a, b) in enumerate(
            [
                (weights, wx.at[:, :, pl.ds(0, PTS)]),
                (dep_owner, dow),
                (dep_slot, dsl),
                (nbr_elem, nel),
                (nbr_edge, ned),
                (metric, met),
            ]
        )
    ]
    load_t = [pltpu.make_async_copy(tracers.at[:, k], own_t.at[k], loc_t.at[0, k]) for k in range(LEV)]
    load_s = [pltpu.make_async_copy(sources.at[:, k], src.at[k], loc_t.at[1, k]) for k in range(LEV)]

    def ex1(k, side):
        return remote(own_t.at[k], f1.at[k, side], send1.at[k, side], recv1.at[k, side], side)

    def ex2(k, side):
        return remote(first.at[k], f2.at[k, side], send2.at[k, side], recv2.at[k, side], side)

    def ex_w(side):
        return remote(wx, wx_in.at[side], sendm.at[0, side], recvm.at[0, side], side)

    def ex_v(side):
        return remote(v_out.at[side], v_in.at[side], sendm.at[1, side], recvm.at[1, side], side)

    def ex_s(side):
        return remote(sm.at[side], sm_in.at[side], sendm.at[2, side], recvm.at[2, side], side)

    def ex_p(k, side):
        return remote(once.at[k, side], once_in.at[k, side], sendp.at[k, side], recvp.at[k, side], side)

    def ex_q(k, side):
        return remote(twice.at[k, side], twice_in.at[k, side], sendq.at[k, side], recvq.at[k, side], side)

    barrier = pltpu.get_barrier_semaphore()
    for side in range(2):
        pl.semaphore_signal(
            barrier, inc=1, device_id=(beyond(side),), device_id_type=pl.DeviceIdType.MESH
        )
    for c in load_t:
        c.start()
    for c in small:
        c.start()
    for c in load_s:
        c.start()
    for c in load_t:
        c.wait()
    pl.semaphore_wait(barrier, 2)
    for k in range(LEV):
        for side in range(2):
            ex1(k, side).start()

    for c in small:
        c.wait()
    wx[:, :, pl.ds(PTS, 128)] = jnp.zeros((16, LEV, 128), F32)
    for e in range(16):
        code = offset_of(dow[e], me, count) * 16 + dsl[e]
        wx[e, :, pl.ds(PTS, 16)] = code.astype(F32)
    for c in load_s:
        c.wait()
    diagonal = (cols((16, PTS)) >> 4) == rows((16, PTS))
    eye16 = cols((16, 16)) == rows((16, 16))
    tile_j = ((rows((PTS, PTS)) & 15) == (cols((PTS, PTS)) & 15)).astype(F32).astype(BF16)
    lane_elem = (cols((1, PTS)) >> 4).astype(F32)

    def tiled(table, k):
        his, los, codes = [], [], []
        for e in range(16):
            row = table[e, pl.ds(k, 1), pl.ds(0, PTS)]
            hi = row.astype(BF16).astype(F32)
            his.append(jnp.where(diagonal, jnp.broadcast_to(hi, (16, PTS)), 0.0))
            los.append(jnp.where(diagonal, jnp.broadcast_to(row - hi, (16, PTS)), 0.0))
            code = table[e, pl.ds(k, 1), pl.ds(PTS, 16)]
            codes.append(jnp.where(eye16, jnp.broadcast_to(code, (16, 16)), 0.0))
        hi = dot(jnp.concatenate(his, axis=0).astype(BF16), tile_j)
        lo = dot(jnp.concatenate(los, axis=0).astype(BF16), tile_j)
        code = jnp.sum(jnp.concatenate(codes, axis=0), axis=1, keepdims=True)
        return hi, lo, code

    def mix(k, i, field):
        hi, lo = split(field.reshape(PTS, Q))
        return dot3(w_hi[k, i], w_lo[k, i], hi, lo)

    def cube(x):
        return x.reshape(16, 16, Q)

    for k in range(LEV):
        hi, lo, code = tiled(wx, k)
        for i in range(3):
            match = code == (lane_elem + float(16 * i))
            w_hi[k, i] = jnp.where(match, hi, 0.0).astype(BF16)
            w_lo[k, i] = jnp.where(match, lo, 0.0).astype(BF16)
        first[k] = cube(mix(k, 1, own_t[k])) + src[k]

    square = (PTS, PTS)
    r, c = rows(square), cols(square)
    same_elem = (r >> 4) == (c >> 4)
    unit = r == c
    left_a, left_b = direction_table((16, 16), False), direction_table((16, 16), True)
    right_a, right_b = direction_table((16, PTS), False), direction_table((16, PTS), True)
    fa, fb = [], []
    for e in range(16):
        fa.append(left_a * jnp.broadcast_to(met[e, pl.ds(0, 1), :], (16, 16)))
        fb.append(left_b * jnp.broadcast_to(met[e, pl.ds(1, 1), :], (16, 16)))
    full = dot_split(jnp.concatenate(fa, axis=0), right_a) + dot_split(jnp.concatenate(fb, axis=0), right_b)
    m = jnp.where(same_elem, full, 0.0)

    edge_row, edge_col = rows((PTS, 16)), cols((PTS, 16))

    def edge_column(table):
        spread_out = jnp.zeros((PTS, 16), F32)
        for s in range(4):
            here = ((edge_row >> 4) == edge_col) & (((edge_row >> 2) & 3) == s)
            line = table[pl.ds(s, 1), :].astype(F32)
            spread_out = jnp.where(here, jnp.broadcast_to(line, (PTS, 16)), spread_out)
        return jnp.sum(spread_out, axis=1, keepdims=True).astype(I32)

    ne, nt = edge_column(nel), edge_column(ned)
    off = offset_of(ne >> 4, me, count)
    pe = (ne & 15) * 4 + nt
    off_f, pe_f = off.astype(F32), pe.astype(F32)
    off_row = jnp.sum(jnp.where(unit, off_f, 0.0), axis=0, keepdims=True)
    pe_row = jnp.sum(jnp.where(unit, pe_f, 0.0), axis=0, keepdims=True)
    peer = (off_row == off_f) & ((c & 3) == 0)
    rank_own = jnp.sum(jnp.where(peer & ((c >> 2) < (r >> 2)), 1.0, 0.0), axis=1, keepdims=True).astype(I32)
    rank_pe = jnp.sum(jnp.where(peer & (pe_row < pe_f), 1.0, 0.0), axis=1, keepdims=True).astype(I32)
    point = rows((PTS, 1)) & 3
    slot = jnp.where(off == 1, pe, jnp.where(off == 0, 64 + rank_pe, 80 + rank_pe))
    take = (cols((PTS, 384)) == slot * 4 + 3 - point).astype(F32).astype(BF16)
    place = jnp.where(off == 1, -1, jnp.where(off == 2, 0, 64) + rank_own * 4 + point)
    pack_t = (cols((PTS, 128)) == place).astype(F32)
    pack = pack_t.T.astype(BF16)
    spread_t = (same_elem & ((r & 15) == edge_point((c >> 2) & 3, c & 3))).astype(F32).astype(BF16)
    spread = (same_elem & ((c & 15) == edge_point((r >> 2) & 3, r & 3))).astype(F32).astype(BF16)
    a, b = (rows((PTS, 1)) >> 2) & 3, rows((PTS, 1)) & 3
    rim_a, rim_b = ((a == 0) | (a == 3)).astype(F32), ((b == 0) | (b == 3)).astype(F32)
    counts = 1.0 + rim_a + rim_b
    added = dot(spread_t, take)
    own_add = dot(added[:, :PTS].astype(BF16), spread)
    r_own = (jnp.where(unit, 1.0, 0.0) + own_add) / counts
    r_out = added[:, PTS:] / counts
    picked = dot(pack, spread)
    km = dot_split(picked, m)
    g = dot_split(r_own, m)
    v = dot_split(km, r_out)
    v_out[0] = v[:64]
    v_out[1] = v[64:]
    for side, through in enumerate((v[:64, :64], v[64:, 64:])):
        hi, lo = split(through)
        vz_hi[side] = hi
        vz_lo[side] = lo
    kmg = dot_split(km, g)
    sm[0] = jnp.concatenate([km[:64], kmg[:64]], axis=0)
    sm[1] = jnp.concatenate([km[64:], kmg[64:]], axis=0)

    def hand_matrices():
        for side in range(2):
            ex_w(side).start()
            ex_v(side).start()
            ex_s(side).start()

    pl.when(edge)(hand_matrices)
    for side in range(2):
        hi, lo = split(sm[side])
        sm_hi[side] = hi
        sm_lo[side] = lo
    gr = dot_split(g, r_out)
    gg = dot_split(g, g)
    ext = -VISCOSITY * jnp.concatenate([gr[:, :64], r_out[:, :64], gr[:, 64:], r_out[:, 64:]], axis=1)
    hi, lo = split(ext)
    e_hi[...] = hi
    e_lo[...] = lo

    def neighbour_matrices(side):
        ex_w(side).wait_recv()
        shift = jnp.where(side == 0, 32.0, 0.0)
        for k in range(LEV):
            hi, lo, code = tiled(wx_in.at[side], k)
            match = code == (lane_elem + shift)
            nb_hi[k, side] = jnp.where(match, hi, 0.0).astype(BF16)
            nb_lo[k, side] = jnp.where(match, lo, 0.0).astype(BF16)

    def corrections(side):
        ex_s(side).wait_recv()
        hi, lo = split(sm_in[side])
        sn_hi[side] = hi
        sn_lo[side] = lo
        for k in range(LEV):
            hi, lo = split(first[k].reshape(PTS, Q))
            taken = dot3(nb_hi[k, side], nb_lo[k, side], hi, lo)
            hi, lo = split(taken)
            corr[k, side] = dot3(sn_hi[side], sn_lo[side], hi, lo)

    def second_from(k, side, last):
        ex2(k, side).wait_recv()
        part = mix(k, 2 * side, f2[k, side])
        here = base[k]
        hi, lo = split(here + part)
        terms = dot3(sm_hi[side], sm_lo[side], hi, lo)
        once[k, side] = terms[:64]
        twice_own[k, side] = terms[64:]
        ex_p(k, side).start()
        if last:
            hi, lo = split(total[k] + part)
            total[k] = dot3(h_hi[...], h_lo[...], hi, lo)
        else:
            total[k] = here + part

    def relay(k, side):
        ex_p(k, side).wait_recv()
        whole = once_in[k, side] + corr[k, side, pl.ds(0, 64)]
        terms_in[k, side, pl.ds(0, 64)] = whole
        hi, lo = split(whole)
        twice[k, side] = twice_own[k, side] + dot3(vz_hi[side], vz_lo[side], hi, lo)
        ex_q(k, side).start()

    for k in range(LEV):
        value = first[k].reshape(PTS, Q)
        for side in range(2):
            ex1(k, side).wait_recv()
            value = value + mix(k, 2 * side, f1[k, side])
        first[k] = cube(value)
        for side in range(2):
            ex2(k, side).start()
        base[k] = mix(k, 1, value) + src[k].reshape(PTS, Q)

        @pl.when(edge)
        def _():
            if k >= 1:
                second_from(k - 1, near, False)
            if k == 2:
                neighbour_matrices(near)

    @pl.when(edge)
    def _():
        second_from(LEV - 1, near, False)

    @pl.when(jnp.logical_not(edge))
    def _():
        hand_matrices()
        for k in range(LEV):
            second_from(k, near, False)
        neighbour_matrices(near)

    corrections(near)

    @pl.when(jnp.logical_not(middle))
    def _():
        for k in range(LEV):
            relay(k, near)

    neighbour_matrices(far)
    corrections(far)
    for side in range(2):
        ex_v(side).wait_recv()
    from_prev, from_next = v_in[0], v_in[1]
    none = jnp.zeros((64, 64), F32)
    blocks = jnp.concatenate(
        [
            jnp.concatenate([none, from_prev[:, 64:]], axis=1),
            jnp.concatenate([from_next[:, :64], none], axis=1),
        ],
        axis=0,
    )
    h = jnp.where(unit, 1.0, 0.0) - VISCOSITY * (gg + dot_split(dot_split(r_out, blocks), km))
    hi, lo = split(h)
    h_hi[...] = hi
    h_lo[...] = lo

    def finish(k):
        for side in range(2):
            ex_q(k, side).wait_recv()
            terms_in[k, side, pl.ds(64, 64)] = twice_in[k, side] + corr[k, side, pl.ds(64, 64)]
        hi, lo = split(terms_in[k].reshape(PTS, Q))
        outbuf[:, k] = cube(total[k] + dot3(e_hi[...], e_lo[...], hi, lo))

    for j in range(LEV + 1):
        if j < LEV:
            second_from(j, far, True)
        if j >= 1:
            relay(j - 1, far)

            @pl.when(middle)
            def _():
                relay(j - 1, near)

    for k in range(LEV):
        finish(k)
    for side in range(2):
        ex_w(side).wait_send()
        ex_v(side).wait_send()
        ex_s(side).wait_send()
        for k in range(LEV):
            for send in (ex1, ex2, ex_p, ex_q):
                send(k, side).wait_send()


def local(tracers, sources, weights, dep_owner, dep_slot, nbr_elem, nbr_edge, metric):
    count = lax.axis_size("elem")
    block = (LEV, 16, 16, Q)
    dma = pltpu.SemaphoreType.DMA
    vmem = pltpu.VMEM
    pairs = (LEV, 2, 16, 16, Q)
    flat = (LEV, PTS, Q)
    tall = (2, 128, PTS)
    slim = (LEV, 2, 64, Q)
    scratch = [
        vmem(block, F32), vmem(block, F32), vmem((16, LEV, 384), F32),
        vmem(dep_owner.shape, I32), vmem(dep_slot.shape, I32),
        vmem(nbr_elem.shape[::-1], I32), vmem(nbr_edge.shape[::-1], I32), vmem(metric.shape, F32),
        vmem(pairs, F32), vmem(block, F32), vmem(pairs, F32), vmem(flat, F32), vmem(flat, F32),
        vmem((LEV, 3, PTS, PTS), BF16), vmem((LEV, 3, PTS, PTS), BF16),
        vmem((2, 16, LEV, 384), F32), vmem((LEV, 2, PTS, PTS), BF16), vmem((LEV, 2, PTS, PTS), BF16),
        vmem((2, 64, 128), F32), vmem((2, 64, 128), F32),
        vmem(tall, F32), vmem(tall, BF16), vmem(tall, BF16),
        vmem(tall, F32), vmem(tall, BF16), vmem(tall, BF16),
        vmem((LEV, 2, 128, Q), F32), vmem((2, 64, 64), BF16), vmem((2, 64, 64), BF16),
        vmem(slim, F32), vmem(slim, F32), vmem(slim, F32), vmem(slim, F32), vmem(slim, F32),
        vmem((LEV, 2, 128, Q), F32),
        vmem((PTS, PTS), BF16), vmem((PTS, PTS), BF16),
        vmem((PTS, PTS), BF16), vmem((PTS, PTS), BF16),
        dma((6,)), dma((2, LEV)),
        dma((LEV, 2)), dma((LEV, 2)), dma((LEV, 2)), dma((LEV, 2)), dma((3, 2)), dma((3, 2)),
        dma((LEV, 2)), dma((LEV, 2)), dma((LEV, 2)), dma((LEV, 2)),
    ]
    return pl.pallas_call(
        functools.partial(kernel, count),
        out_shape=pltpu.VMEM(tracers.shape, F32),
        in_specs=[pl.BlockSpec(memory_space=pl.ANY)] * 8,
        out_specs=pl.BlockSpec(memory_space=pltpu.VMEM),
        scratch_shapes=scratch,
        compiler_params=pltpu.CompilerParams(collective_id=0, has_side_effects=True),
        name="tracer_step",
    )(tracers, sources, weights, dep_owner, dep_slot, nbr_elem.T, nbr_edge.T, metric)


def solution(mesh):
    placed = (
        P("elem", None, None, None),
        P("elem", None, None, None),
        P("elem", None, None),
        P("elem", None, None),
        P("elem", None, None),
        P("elem", None),
        P("elem", None),
        P("elem", None, None),
    )
    return jax.shard_map(
        local, mesh=mesh, in_specs=placed, out_specs=P("elem", None, None, None), check_vma=False
    )
```

```python
import functools

import jax
import jax.numpy as jnp
import numpy as np
from jax import lax
from jax.experimental import pallas as pl
from jax.experimental.pallas import tpu as pltpu
from jax.sharding import PartitionSpec as P

VISCOSITY = 0.002
LEV = 4
PTS = 256
Q = 128
F32 = jnp.float32
BF16 = jnp.bfloat16
I32 = jnp.int32


def derivative_matrix():
    nodes = np.array([-1.0, -np.sqrt(0.2), np.sqrt(0.2), 1.0])
    count = nodes.shape[0]
    bary = np.array(
        [1.0 / np.prod([nodes[j] - nodes[m] for m in range(count) if m != j]) for j in range(count)]
    )
    derivative = np.zeros((count, count))
    for i in range(count):
        for j in range(count):
            if i != j:
                derivative[i, j] = bary[j] / bary[i] / (nodes[i] - nodes[j])
        derivative[i, i] = -np.sum(derivative[i])
    return derivative


def rows(shape):
    return lax.broadcasted_iota(I32, shape, 0)


def cols(shape):
    return lax.broadcasted_iota(I32, shape, 1)


def dot(a, b):
    return jnp.dot(a, b, preferred_element_type=F32)


def split(x):
    hi = x.astype(BF16)
    lo = (x - hi.astype(F32)).astype(BF16)
    return hi, lo


def dot3(a_hi, a_lo, b_hi, b_lo):
    n = b_hi.shape[1]
    both = dot(a_hi, jnp.concatenate([b_hi, b_lo], axis=1))
    return both[:, :n] + (both[:, n:] + dot(a_lo, b_hi))


def dot_split(a, b):
    return dot3(*split(a), *split(b))


def edge_point(s, k):
    return jnp.where(s == 0, 4 * k, jnp.where(s == 1, 12 + k, jnp.where(s == 2, 15 - 4 * k, 3 - k)))


def direction_table(shape, along_b):
    m, p = rows(shape) & 15, cols(shape) & 15
    if along_b:
        i, j, live = m & 3, p & 3, (m >> 2) == (p >> 2)
    else:
        i, j, live = m >> 2, p >> 2, (m & 3) == (p & 3)
    which = jnp.where(live, i * 4 + j, -1)
    table = derivative_matrix()
    value = jnp.zeros(shape, F32)
    for at in range(16):
        value = jnp.where(which == at, np.float32(table[at // 4, at % 4]), value)
    return value


def offset_of(owner, me, count):
    d = owner - me
    d = jnp.where(d > 1, d - count, d)
    d = jnp.where(d < -1, d + count, d)
    return d + 1


def kernel(
    count,
    tracers, sources, weights, dep_owner, dep_slot, nbr_elem, nbr_edge, metric,
    outbuf,
    own_t, src, wx, dow, dsl, nel, ned, met,
    f1, first, f2, base, total,
    w_hi, w_lo, wx_in, nb_hi, nb_lo,
    v_out, v_in, sm, sm_hi, sm_lo, sm_in, sn_hi, sn_lo,
    corr, vz_hi, vz_lo, once, twice_own, twice, once_in, twice_in, terms_in,
    h_hi, h_lo, e_hi, e_lo,
    loc, loc_t,
    sent, recv1, recv2, recvm, recvp, recvq,
):
    me = lax.axis_index("elem")
    place_in_row = lax.rem(me, 8)
    near = jnp.where(place_in_row < 4, 1, 0)
    far = 1 - near
    edge = (place_in_row == 0) | (place_in_row == 7)
    middle = (place_in_row == 3) | (place_in_row == 4)
    ahead = jnp.where(middle, far, near)

    def beyond(side):
        return lax.rem(me + 1 - 2 * side + count, count)

    def remote(source, target, send_sem, recv_sem, side):
        return pltpu.make_async_remote_copy(
            src_ref=source,
            dst_ref=target,
            send_sem=send_sem,
            recv_sem=recv_sem,
            device_id=(beyond(side),),
            device_id_type=pl.DeviceIdType.MESH,
        )

    small = [
        pltpu.make_async_copy(a, b, loc.at[i])
        for i, (a, b) in enumerate(
            [
                (weights, wx.at[:, :, pl.ds(0, PTS)]),
                (dep_owner, dow),
                (dep_slot, dsl),
                (nbr_elem, nel),
                (nbr_edge, ned),
                (metric, met),
            ]
        )
    ]
    load_t = [pltpu.make_async_copy(tracers.at[:, k], own_t.at[k], loc_t.at[0]) for k in range(LEV)]
    load_s = [pltpu.make_async_copy(sources.at[:, k], src.at[k], loc_t.at[1]) for k in range(LEV)]

    def wait_bytes(like, semaphore):
        pltpu.make_async_copy(like, like, semaphore).wait()

    def ex1(k, side):
        return remote(own_t.at[k], f1.at[k, side], sent.at[side], recv1.at[k, side], side)

    def ex2(k, side):
        return remote(first.at[k], f2.at[k, side], sent.at[side], recv2.at[k, side], side)

    def ex_w(side):
        return remote(wx, wx_in.at[side], sent.at[side], recvm.at[side], side)

    def ex_v(side):
        return remote(v_out.at[side], v_in.at[side], sent.at[side], recvm.at[side], side)

    def ex_s(side):
        return remote(sm.at[side], sm_in.at[side], sent.at[side], recvm.at[side], side)

    def ex_p(k, side):
        return remote(once.at[k, side], once_in.at[k, side], sent.at[side], recvp.at[k, side], side)

    def ex_q(k, side):
        return remote(twice.at[k, side], twice_in.at[k, side], sent.at[side], recvq.at[k], side)

    barrier = pltpu.get_barrier_semaphore()
    for side in range(2):
        pl.semaphore_signal(
            barrier, inc=1, device_id=(beyond(side),), device_id_type=pl.DeviceIdType.MESH
        )
    for c in load_t:
        c.start()
    for c in small:
        c.start()
    for c in load_s:
        c.start()
    wait_bytes(own_t, loc_t.at[0])
    pl.semaphore_wait(barrier, 2)
    for k in range(LEV):
        for side in range(2):
            ex1(k, side).start()

    for c in small:
        c.wait()
    wx[:, :, pl.ds(PTS, 128)] = jnp.zeros((16, LEV, 128), F32)
    for e in range(16):
        code = offset_of(dow[e], me, count) * 16 + dsl[e]
        wx[e, :, pl.ds(PTS, 16)] = code.astype(F32)
    wait_bytes(src, loc_t.at[1])
    diagonal = (cols((16, PTS)) >> 4) == rows((16, PTS))
    eye16 = cols((16, 16)) == rows((16, 16))
    tile_j = ((rows((PTS, PTS)) & 15) == (cols((PTS, PTS)) & 15)).astype(F32).astype(BF16)
    lane_elem = (cols((1, PTS)) >> 4).astype(F32)

    def tiled(table, k):
        his, los, codes = [], [], []
        for e in range(16):
            row = table[e, pl.ds(k, 1), pl.ds(0, PTS)]
            hi = row.astype(BF16).astype(F32)
            his.append(jnp.where(diagonal, jnp.broadcast_to(hi, (16, PTS)), 0.0))
            los.append(jnp.where(diagonal, jnp.broadcast_to(row - hi, (16, PTS)), 0.0))
            code = table[e, pl.ds(k, 1), pl.ds(PTS, 16)]
            codes.append(jnp.where(eye16, jnp.broadcast_to(code, (16, 16)), 0.0))
        hi = dot(jnp.concatenate(his, axis=0).astype(BF16), tile_j)
        lo = dot(jnp.concatenate(los, axis=0).astype(BF16), tile_j)
        code = jnp.sum(jnp.concatenate(codes, axis=0), axis=1, keepdims=True)
        return hi, lo, code

    def mix(k, i, field):
        hi, lo = split(field.reshape(PTS, Q))
        return dot3(w_hi[k, i], w_lo[k, i], hi, lo)

    def cube(x):
        return x.reshape(16, 16, Q)

    for k in range(LEV):
        hi, lo, code = tiled(wx, k)
        for i in range(3):
            match = code == (lane_elem + float(16 * i))
            w_hi[k, i] = jnp.where(match, hi, 0.0).astype(BF16)
            w_lo[k, i] = jnp.where(match, lo, 0.0).astype(BF16)
        first[k] = cube(mix(k, 1, own_t[k])) + src[k]

    square = (PTS, PTS)
    r, c = rows(square), cols(square)
    same_elem = (r >> 4) == (c >> 4)
    unit = r == c
    left_a, left_b = direction_table((16, 16), False), direction_table((16, 16), True)
    right_a, right_b = direction_table((16, PTS), False), direction_table((16, PTS), True)
    fa, fb = [], []
    for e in range(16):
        fa.append(left_a * jnp.broadcast_to(met[e, pl.ds(0, 1), :], (16, 16)))
        fb.append(left_b * jnp.broadcast_to(met[e, pl.ds(1, 1), :], (16, 16)))
    full = dot_split(jnp.concatenate(fa, axis=0), right_a) + dot_split(jnp.concatenate(fb, axis=0), right_b)
    m = jnp.where(same_elem, full, 0.0)

    edge_row, edge_col = rows((PTS, 16)), cols((PTS, 16))

    def edge_column(table):
        spread_out = jnp.zeros((PTS, 16), F32)
        for s in range(4):
            here = ((edge_row >> 4) == edge_col) & (((edge_row >> 2) & 3) == s)
            line = table[pl.ds(s, 1), :].astype(F32)
            spread_out = jnp.where(here, jnp.broadcast_to(line, (PTS, 16)), spread_out)
        return jnp.sum(spread_out, axis=1, keepdims=True).astype(I32)

    ne, nt = edge_column(nel), edge_column(ned)
    off = offset_of(ne >> 4, me, count)
    pe = (ne & 15) * 4 + nt
    off_f, pe_f = off.astype(F32), pe.astype(F32)
    off_row = jnp.sum(jnp.where(unit, off_f, 0.0), axis=0, keepdims=True)
    pe_row = jnp.sum(jnp.where(unit, pe_f, 0.0), axis=0, keepdims=True)
    peer = (off_row == off_f) & ((c & 3) == 0)
    rank_own = jnp.sum(jnp.where(peer & ((c >> 2) < (r >> 2)), 1.0, 0.0), axis=1, keepdims=True).astype(I32)
    rank_pe = jnp.sum(jnp.where(peer & (pe_row < pe_f), 1.0, 0.0), axis=1, keepdims=True).astype(I32)
    point = rows((PTS, 1)) & 3
    slot = jnp.where(off == 1, pe, jnp.where(off == 0, 64 + rank_pe, 80 + rank_pe))
    take = (cols((PTS, 384)) == slot * 4 + 3 - point).astype(F32).astype(BF16)
    place = jnp.where(off == 1, -1, jnp.where(off == 2, 0, 64) + rank_own * 4 + point)
    pack_t = (cols((PTS, 128)) == place).astype(F32)
    pack = pack_t.T.astype(BF16)
    spread_t = (same_elem & ((r & 15) == edge_point((c >> 2) & 3, c & 3))).astype(F32).astype(BF16)
    spread = (same_elem & ((c & 15) == edge_point((r >> 2) & 3, r & 3))).astype(F32).astype(BF16)
    a, b = (rows((PTS, 1)) >> 2) & 3, rows((PTS, 1)) & 3
    rim_a, rim_b = ((a == 0) | (a == 3)).astype(F32), ((b == 0) | (b == 3)).astype(F32)
    counts = 1.0 + rim_a + rim_b
    added = dot(spread_t, take)
    own_add = dot(added[:, :PTS].astype(BF16), spread)
    r_own = (jnp.where(unit, 1.0, 0.0) + own_add) / counts
    r_out = added[:, PTS:] / counts
    picked = dot(pack, spread)
    km = dot_split(picked, m)
    g = dot_split(r_own, m)
    v = dot_split(km, r_out)
    v_out[0] = v[:64]
    v_out[1] = v[64:]
    for side, through in enumerate((v[:64, :64], v[64:, 64:])):
        hi, lo = split(through)
        vz_hi[side] = hi
        vz_lo[side] = lo
    kmg = dot_split(km, g)
    sm[0] = jnp.concatenate([km[:64], kmg[:64]], axis=0)
    sm[1] = jnp.concatenate([km[64:], kmg[64:]], axis=0)

    def hand_matrices():
        for side in range(2):
            ex_w(side).start()
            ex_s(side).start()
            ex_v(side).start()

    pl.when(edge)(hand_matrices)
    for side in range(2):
        hi, lo = split(sm[side])
        sm_hi[side] = hi
        sm_lo[side] = lo
    gr = dot_split(g, r_out)
    gg = dot_split(g, g)
    ext = -VISCOSITY * jnp.concatenate([gr[:, :64], r_out[:, :64], gr[:, 64:], r_out[:, 64:]], axis=1)
    hi, lo = split(ext)
    e_hi[...] = hi
    e_lo[...] = lo

    def meet(side):
        wait_bytes(first.at[pl.ds(0, 2)], recvm.at[side])
        shift = jnp.where(side == 0, 32.0, 0.0)
        for k in range(LEV):
            hi, lo, code = tiled(wx_in.at[side], k)
            match = code == (lane_elem + shift)
            nb_hi[k, side] = jnp.where(match, hi, 0.0).astype(BF16)
            nb_lo[k, side] = jnp.where(match, lo, 0.0).astype(BF16)
        hi, lo = split(sm_in[side])
        sn_hi[side] = hi
        sn_lo[side] = lo

    def correct(k, side):
        hi, lo = split(first[k].reshape(PTS, Q))
        taken = dot3(nb_hi[k, side], nb_lo[k, side], hi, lo)
        hi, lo = split(taken)
        corr[k, side] = dot3(sn_hi[side], sn_lo[side], hi, lo)

    def second_from(k, side, start):
        ex2(k, side).wait_recv()
        part = mix(k, 2 * side, f2[k, side])
        here = base[k]
        hi, lo = split(here + part)
        terms = dot3(sm_hi[side], sm_lo[side], hi, lo)
        once[k, side] = terms[:64]
        twice_own[k, side] = terms[64:]
        ex_p(k, side).start()
        total[k] = (here if start else total[k]) + part

    def settle(k):
        hi, lo = split(total[k])
        total[k] = dot3(h_hi[...], h_lo[...], hi, lo)

    def relay(k, side):
        ex_p(k, side).wait_recv()
        whole = once_in[k, side] + corr[k, side, pl.ds(0, 64)]
        terms_in[k, side, pl.ds(0, 64)] = whole
        hi, lo = split(whole)
        twice[k, side] = twice_own[k, side] + dot3(vz_hi[side], vz_lo[side], hi, lo)
        ex_q(k, side).start()

    for k in range(LEV):
        value = first[k].reshape(PTS, Q)
        for side in range(2):
            ex1(k, side).wait_recv()
            value = value + mix(k, 2 * side, f1[k, side])
        first[k] = cube(value)
        for side in range(2):
            ex2(k, side).start()
        base[k] = mix(k, 1, value) + src[k].reshape(PTS, Q)

        @pl.when(edge)
        def _():
            if k >= 1:
                second_from(k - 1, near, True)
            if k == 1:
                meet(near)
            if k == 2:
                correct(0, near)
            if k >= 2:
                correct(k - 1, near)
                relay(k - 2, near)

    @pl.when(edge)
    def _():
        second_from(LEV - 1, near, True)
        correct(LEV - 1, near)
        for k in (LEV - 2, LEV - 1):
            relay(k, near)

    @pl.when(jnp.logical_not(edge))
    def _():
        hand_matrices()
        for k in range(LEV):
            second_from(k, ahead, True)
        for k in range(LEV):
            second_from(k, 1 - ahead, False)
        meet(near)
        for k in range(LEV):
            correct(k, near)
            relay(k, near)

    meet(far)
    for k in range(LEV):
        correct(k, far)
    from_prev, from_next = v_in[0], v_in[1]
    none = jnp.zeros((64, 64), F32)
    blocks = jnp.concatenate(
        [
            jnp.concatenate([none, from_prev[:, 64:]], axis=1),
            jnp.concatenate([from_next[:, :64], none], axis=1),
        ],
        axis=0,
    )
    h = jnp.where(unit, 1.0, 0.0) - VISCOSITY * (gg + dot_split(dot_split(r_out, blocks), km))
    hi, lo = split(h)
    h_hi[...] = hi
    h_lo[...] = lo

    def finish(k):
        wait_bytes(twice_in.at[k], recvq.at[k])
        for side in range(2):
            terms_in[k, side, pl.ds(64, 64)] = twice_in[k, side] + corr[k, side, pl.ds(64, 64)]
        hi, lo = split(terms_in[k].reshape(PTS, Q))
        outbuf[:, k] = cube(total[k] + dot3(e_hi[...], e_lo[...], hi, lo))

    @pl.when(edge)
    def _():
        for j in range(LEV + 1):
            if j < LEV:
                second_from(j, far, False)
            if j >= 1:
                relay(j - 1, far)
                settle(j - 1)
        for k in range(LEV - 1):
            finish(k)

    @pl.when(jnp.logical_not(edge))
    def _():
        for k in range(LEV):
            settle(k)
        for k in range(LEV):
            relay(k, far)
        for k in range(LEV - 1):
            finish(k)

    finish(LEV - 1)
    for side in range(2):
        wait_bytes(w_hi, sent.at[side])


def local(tracers, sources, weights, dep_owner, dep_slot, nbr_elem, nbr_edge, metric):
    count = lax.axis_size("elem")
    block = (LEV, 16, 16, Q)
    dma = pltpu.SemaphoreType.DMA
    vmem = pltpu.VMEM
    pairs = (LEV, 2, 16, 16, Q)
    flat = (LEV, PTS, Q)
    tall = (2, 128, PTS)
    slim = (LEV, 2, 64, Q)
    scratch = [
        vmem(block, F32), vmem(block, F32), vmem((16, LEV, 384), F32),
        vmem(dep_owner.shape, I32), vmem(dep_slot.shape, I32),
        vmem(nbr_elem.shape[::-1], I32), vmem(nbr_edge.shape[::-1], I32), vmem(metric.shape, F32),
        vmem(pairs, F32), vmem(block, F32), vmem(pairs, F32), vmem(flat, F32), vmem(flat, F32),
        vmem((LEV, 3, PTS, PTS), BF16), vmem((LEV, 3, PTS, PTS), BF16),
        vmem((2, 16, LEV, 384), F32), vmem((LEV, 2, PTS, PTS), BF16), vmem((LEV, 2, PTS, PTS), BF16),
        vmem((2, 64, 128), F32), vmem((2, 64, 128), F32),
        vmem(tall, F32), vmem(tall, BF16), vmem(tall, BF16),
        vmem(tall, F32), vmem(tall, BF16), vmem(tall, BF16),
        vmem((LEV, 2, 128, Q), F32), vmem((2, 64, 64), BF16), vmem((2, 64, 64), BF16),
        vmem(slim, F32), vmem(slim, F32), vmem(slim, F32), vmem(slim, F32), vmem(slim, F32),
        vmem((LEV, 2, 128, Q), F32),
        vmem((PTS, PTS), BF16), vmem((PTS, PTS), BF16),
        vmem((PTS, PTS), BF16), vmem((PTS, PTS), BF16),
        dma((6,)), dma((2,)),
        dma((2,)), dma((LEV, 2)), dma((LEV, 2)), dma((2,)), dma((LEV, 2)), dma((LEV,)),
    ]
    return pl.pallas_call(
        functools.partial(kernel, count),
        out_shape=pltpu.VMEM(tracers.shape, F32),
        in_specs=[pl.BlockSpec(memory_space=pl.ANY)] * 8,
        out_specs=pl.BlockSpec(memory_space=pltpu.VMEM),
        scratch_shapes=scratch,
        compiler_params=pltpu.CompilerParams(collective_id=0, has_side_effects=True),
        name="tracer_step",
    )(tracers, sources, weights, dep_owner, dep_slot, nbr_elem.T, nbr_edge.T, metric)


def solution(mesh):
    placed = (
        P("elem", None, None, None),
        P("elem", None, None, None),
        P("elem", None, None),
        P("elem", None, None),
        P("elem", None, None),
        P("elem", None),
        P("elem", None),
        P("elem", None, None),
    )
    return jax.shard_map(
        local, mesh=mesh, in_specs=placed, out_specs=P("elem", None, None, None), check_vma=False
    )
```

```python
import functools

import jax
import jax.numpy as jnp
import numpy as np
from jax import lax
from jax.experimental import pallas as pl
from jax.experimental.pallas import tpu as pltpu
from jax.sharding import PartitionSpec as P

VISCOSITY = 0.002
LEV = 4
PTS = 256
Q = 128
F32 = jnp.float32
BF16 = jnp.bfloat16
I32 = jnp.int32


def derivative_matrix():
    nodes = np.array([-1.0, -np.sqrt(0.2), np.sqrt(0.2), 1.0])
    count = nodes.shape[0]
    bary = np.array(
        [1.0 / np.prod([nodes[j] - nodes[m] for m in range(count) if m != j]) for j in range(count)]
    )
    derivative = np.zeros((count, count))
    for i in range(count):
        for j in range(count):
            if i != j:
                derivative[i, j] = bary[j] / bary[i] / (nodes[i] - nodes[j])
        derivative[i, i] = -np.sum(derivative[i])
    return derivative


def rows(shape):
    return lax.broadcasted_iota(I32, shape, 0)


def cols(shape):
    return lax.broadcasted_iota(I32, shape, 1)


def dot(a, b):
    return jnp.dot(a, b, preferred_element_type=F32)


def split(x):
    hi = x.astype(BF16)
    lo = (x - hi.astype(F32)).astype(BF16)
    return hi, lo


def dot3(a_hi, a_lo, b_hi, b_lo):
    n = b_hi.shape[1]
    both = dot(a_hi, jnp.concatenate([b_hi, b_lo], axis=1))
    return both[:, :n] + (both[:, n:] + dot(a_lo, b_hi))


def dot_split(a, b):
    return dot3(*split(a), *split(b))


def edge_point(s, k):
    return jnp.where(s == 0, 4 * k, jnp.where(s == 1, 12 + k, jnp.where(s == 2, 15 - 4 * k, 3 - k)))


def direction_table(shape, along_b):
    m, p = rows(shape) & 15, cols(shape) & 15
    if along_b:
        i, j, live = m & 3, p & 3, (m >> 2) == (p >> 2)
    else:
        i, j, live = m >> 2, p >> 2, (m & 3) == (p & 3)
    which = jnp.where(live, i * 4 + j, -1)
    table = derivative_matrix()
    value = jnp.zeros(shape, F32)
    for at in range(16):
        value = jnp.where(which == at, np.float32(table[at // 4, at % 4]), value)
    return value


def offset_of(owner, me, count):
    d = owner - me
    d = jnp.where(d > 1, d - count, d)
    d = jnp.where(d < -1, d + count, d)
    return d + 1


def kernel(
    count,
    tracers, sources, weights, dep_owner, dep_slot, nbr_elem, nbr_edge, metric,
    outbuf,
    own_t, src, wx, dow, dsl, nel, ned, met,
    f1, own, partial, first, f2, fix, base, total,
    w_hi, w_lo, wx_in, nb_hi, nb_lo, taken_hi, taken_lo, span,
    sm, sm_hi, sm_lo, sm_in, sn_hi, sn_lo,
    corr, vz_hi, vz_lo, once, twice_own, twice, once_in, twice_in, terms_in,
    h_hi, h_lo, e_hi, e_lo, eq_hi, eq_lo, back_hi, back_lo,
    loc, loc_t,
    sent, recv1, recv2, recvm, recvp, recvq,
):
    me = lax.axis_index("elem")
    place_in_row = lax.rem(me, 8)
    near = jnp.where(place_in_row < 4, 1, 0)
    far = 1 - near
    edge = (place_in_row == 0) | (place_in_row == 7)
    twin = jnp.where(lax.rem(me, 2) == 0, 1, 0)
    remote_side = 1 - twin
    middle = (place_in_row == 3) | (place_in_row == 4)
    ahead = jnp.where(middle, far, near)

    def beyond(side):
        return lax.rem(me + 1 - 2 * side + count, count)

    def remote(source, target, send_sem, recv_sem, side):
        return pltpu.make_async_remote_copy(
            src_ref=source,
            dst_ref=target,
            send_sem=send_sem,
            recv_sem=recv_sem,
            device_id=(beyond(side),),
            device_id_type=pl.DeviceIdType.MESH,
        )

    small = [
        pltpu.make_async_copy(a, b, loc.at[i])
        for i, (a, b) in enumerate(
            [
                (weights, wx.at[:, :, pl.ds(0, PTS)]),
                (dep_owner, dow),
                (dep_slot, dsl),
                (nbr_elem, nel),
                (nbr_edge, ned),
                (metric, met),
            ]
        )
    ]
    load_t = [pltpu.make_async_copy(tracers.at[:, k], own_t.at[k], loc_t.at[0]) for k in range(LEV)]
    load_s = [pltpu.make_async_copy(sources.at[:, k], src.at[k], loc_t.at[1]) for k in range(LEV)]

    def wait_bytes(like, semaphore):
        pltpu.make_async_copy(like, like, semaphore).wait()

    def ex1(k, side):
        return remote(own_t.at[k], f1.at[k, side], sent.at[side], recv1.at[k, side], side)

    def ex2(k, side):
        return remote(partial.at[k, side], f2.at[k, side], sent.at[side], recv2.at[k, side], side)

    def ex_w(side):
        return remote(wx, wx_in.at[side], sent.at[side], recvm.at[0, side], side)

    def ex_m(side, part):
        rows_of = pl.ds(64 * part, 64)
        return remote(
            sm.at[side, rows_of], sm_in.at[side, rows_of], sent.at[side], recvm.at[1 + part, side], side
        )

    def ex_p(k, side):
        return remote(once.at[k, side], once_in.at[k, side], sent.at[side], recvp.at[k, side], side)

    def ex_q(k, side):
        return remote(twice.at[k, side], twice_in.at[k, side], sent.at[side], recvq.at[k], side)

    barrier = pltpu.get_barrier_semaphore()
    for side in range(2):
        pl.semaphore_signal(
            barrier, inc=1, device_id=(beyond(side),), device_id_type=pl.DeviceIdType.MESH
        )
    for c in load_t:
        c.start()
    for c in small:
        c.start()
    for c in load_s:
        c.start()
    wait_bytes(own_t, loc_t.at[0])
    pl.semaphore_wait(barrier, 2)
    for k in range(LEV):
        for side in range(2):
            ex1(k, side).start()

    for c in small:
        c.wait()
    wx[:, :, pl.ds(PTS, 128)] = jnp.zeros((16, LEV, 128), F32)
    for e in range(16):
        code = offset_of(dow[e], me, count) * 16 + dsl[e]
        wx[e, :, pl.ds(PTS, 16)] = code.astype(F32)
    for side in range(2):
        ex_w(side).start()
    wait_bytes(src, loc_t.at[1])
    diagonal = (cols((16, PTS)) >> 4) == rows((16, PTS))
    eye16 = cols((16, 16)) == rows((16, 16))
    tile_j = ((rows((PTS, PTS)) & 15) == (cols((PTS, PTS)) & 15)).astype(F32).astype(BF16)
    lane_elem = (cols((1, PTS)) >> 4).astype(F32)

    def tiled(table, k):
        his, los, codes = [], [], []
        for e in range(16):
            row = table[e, pl.ds(k, 1), pl.ds(0, PTS)]
            hi = row.astype(BF16).astype(F32)
            his.append(jnp.where(diagonal, jnp.broadcast_to(hi, (16, PTS)), 0.0))
            los.append(jnp.where(diagonal, jnp.broadcast_to(row - hi, (16, PTS)), 0.0))
            code = table[e, pl.ds(k, 1), pl.ds(PTS, 16)]
            codes.append(jnp.where(eye16, jnp.broadcast_to(code, (16, 16)), 0.0))
        hi = dot(jnp.concatenate(his, axis=0).astype(BF16), tile_j)
        lo = dot(jnp.concatenate(los, axis=0).astype(BF16), tile_j)
        code = jnp.sum(jnp.concatenate(codes, axis=0), axis=1, keepdims=True)
        return hi, lo, code

    def mix(k, i, field):
        hi, lo = split(field.reshape(PTS, Q))
        return dot3(w_hi[k, i], w_lo[k, i], hi, lo)

    def cube(x):
        return x.reshape(16, 16, Q)

    for k in range(LEV):
        hi, lo, code = tiled(wx, k)
        for i in range(3):
            match = code == (lane_elem + float(16 * i))
            w_hi[k, i] = jnp.where(match, hi, 0.0).astype(BF16)
            w_lo[k, i] = jnp.where(match, lo, 0.0).astype(BF16)
        own[k] = mix(k, 1, own_t[k]) + src[k].reshape(PTS, Q)

    square = (PTS, PTS)
    r, c = rows(square), cols(square)
    same_elem = (r >> 4) == (c >> 4)
    unit = r == c
    left_a, left_b = direction_table((16, 16), False), direction_table((16, 16), True)
    right_a, right_b = direction_table((16, PTS), False), direction_table((16, PTS), True)
    fa, fb = [], []
    for e in range(16):
        fa.append(left_a * jnp.broadcast_to(met[e, pl.ds(0, 1), :], (16, 16)))
        fb.append(left_b * jnp.broadcast_to(met[e, pl.ds(1, 1), :], (16, 16)))
    full = dot_split(jnp.concatenate(fa, axis=0), right_a) + dot_split(jnp.concatenate(fb, axis=0), right_b)
    m = jnp.where(same_elem, full, 0.0)

    edge_row, edge_col = rows((PTS, 16)), cols((PTS, 16))

    def edge_column(table):
        spread_out = jnp.zeros((PTS, 16), F32)
        for s in range(4):
            here = ((edge_row >> 4) == edge_col) & (((edge_row >> 2) & 3) == s)
            line = table[pl.ds(s, 1), :].astype(F32)
            spread_out = jnp.where(here, jnp.broadcast_to(line, (PTS, 16)), spread_out)
        return jnp.sum(spread_out, axis=1, keepdims=True).astype(I32)

    ne, nt = edge_column(nel), edge_column(ned)
    off = offset_of(ne >> 4, me, count)
    pe = (ne & 15) * 4 + nt
    off_f, pe_f = off.astype(F32), pe.astype(F32)
    off_row = jnp.sum(jnp.where(unit, off_f, 0.0), axis=0, keepdims=True)
    pe_row = jnp.sum(jnp.where(unit, pe_f, 0.0), axis=0, keepdims=True)
    peer = (off_row == off_f) & ((c & 3) == 0)
    rank_own = jnp.sum(jnp.where(peer & ((c >> 2) < (r >> 2)), 1.0, 0.0), axis=1, keepdims=True).astype(I32)
    rank_pe = jnp.sum(jnp.where(peer & (pe_row < pe_f), 1.0, 0.0), axis=1, keepdims=True).astype(I32)
    point = rows((PTS, 1)) & 3
    slot = jnp.where(off == 1, pe, jnp.where(off == 0, 64 + rank_pe, 80 + rank_pe))
    take = (cols((PTS, 384)) == slot * 4 + 3 - point).astype(F32).astype(BF16)
    place = jnp.where(off == 1, -1, jnp.where(off == 2, 0, 64) + rank_own * 4 + point)
    pack_t = (cols((PTS, 128)) == place).astype(F32)
    pack = pack_t.T.astype(BF16)
    spread_t = (same_elem & ((r & 15) == edge_point((c >> 2) & 3, c & 3))).astype(F32).astype(BF16)
    spread = (same_elem & ((c & 15) == edge_point((r >> 2) & 3, r & 3))).astype(F32).astype(BF16)
    a, b = (rows((PTS, 1)) >> 2) & 3, rows((PTS, 1)) & 3
    rim_a, rim_b = ((a == 0) | (a == 3)).astype(F32), ((b == 0) | (b == 3)).astype(F32)
    counts = 1.0 + rim_a + rim_b
    added = dot(spread_t, take)
    own_add = dot(added[:, :PTS].astype(BF16), spread)
    r_own = (jnp.where(unit, 1.0, 0.0) + own_add) / counts
    r_out = added[:, PTS:] / counts
    picked = dot(pack, spread)
    km = dot_split(picked, m)
    g = dot_split(r_own, m)
    for side, through in enumerate((dot_split(km[:64], r_out[:, :64]), dot_split(km[64:], r_out[:, 64:]))):
        hi, lo = split(through)
        vz_hi[side] = hi
        vz_lo[side] = lo
    lands = ((off != 1) & (c == pe * 4 + 3 - point)).astype(F32).astype(BF16)
    landed = dot(pack, lands).T.astype(BF16)
    r_nb = dot(spread_t, landed) / counts
    for side, back in enumerate((dot_split(r_nb[:, 64:], km[64:]), dot_split(r_nb[:, :64], km[:64]))):
        hi, lo = split(back)
        back_hi[side] = hi
        back_lo[side] = lo
    kmg = dot_split(km, g)
    sm[0] = jnp.concatenate([km[:64], kmg[:64]], axis=0)
    sm[1] = jnp.concatenate([km[64:], kmg[64:]], axis=0)
    for side in range(2):
        hi, lo = split(sm[side])
        sm_hi[side] = hi
        sm_lo[side] = lo
    gr = dot_split(g, r_out)
    gg = dot_split(g, g)
    ext = -VISCOSITY * jnp.concatenate([gr[:, :64], r_out[:, :64], gr[:, 64:], r_out[:, 64:]], axis=1)
    hi, lo = split(ext)
    e_hi[...] = hi
    e_lo[...] = lo
    for side in range(2):
        hi, lo = split(-VISCOSITY * r_out[:, 64 * side : 64 * side + 64])
        eq_hi[side] = hi
        eq_lo[side] = lo

    def meet(side):
        ex_w(side).wait_recv()
        shift = jnp.where(side == 0, 32.0, 0.0)
        for k in range(LEV):
            hi, lo, code = tiled(wx_in.at[side], k)
            match = code == (lane_elem + shift)
            n_hi = jnp.where(match, hi, 0.0).astype(BF16)
            n_lo = jnp.where(match, lo, 0.0).astype(BF16)
            nb_hi[k, side] = n_hi
            nb_lo[k, side] = n_lo
            hi, lo = split(own_t[k].reshape(PTS, Q))
            fix[k, side] = dot3(n_hi, n_lo, hi, lo)

    def matrix_in(side, part):
        ex_m(side, part).wait_recv()
        hi, lo = split(sm_in[side, pl.ds(64 * part, 64)])
        sn_hi[side, part] = hi
        sn_lo[side, part] = lo

    def take(k, side):
        hi, lo = split(first[k])
        hi, lo = split(dot3(nb_hi[k, side], nb_lo[k, side], hi, lo))
        taken_hi[k, side] = hi
        taken_lo[k, side] = lo

    def correct_once(k, side):
        corr[k, side, pl.ds(0, 64)] = dot3(
            sn_hi[side, 0], sn_lo[side, 0], taken_hi[k, side], taken_lo[k, side]
        )

    def correct_twice(side):
        matrix_in(side, 1)
        for k in range(LEV):
            corr[k, side, pl.ds(64, 64)] = dot3(
                sn_hi[side, 1], sn_lo[side, 1], taken_hi[k, side], taken_lo[k, side]
            )

    def second_from(k, side, start):
        ex2(k, side).wait_recv()
        part = mix(k, 2 * side, f2[k, side].reshape(PTS, Q) + fix[k, side])
        here = base[k]
        hi, lo = split(here + part)
        terms = dot3(sm_hi[side], sm_lo[side], hi, lo)
        once[k, side] = terms[:64]
        twice_own[k, side] = terms[64:]
        ex_p(k, side).start()
        total[k] = (here if start else total[k]) + part

    def settle(k):
        hi, lo = split(total[k])
        total[k] = dot3(h_hi[...], h_lo[...], hi, lo)

    def relay(k, side):
        ex_p(k, side).wait_recv()
        whole = once_in[k, side] + corr[k, side, pl.ds(0, 64)]
        terms_in[k, side, pl.ds(0, 64)] = whole
        hi, lo = split(whole)
        twice[k, side] = twice_own[k, side] + dot3(vz_hi[side], vz_lo[side], hi, lo)
        ex_q(k, side).start()

    meet(twin)
    for k in range(LEV):
        ex1(k, twin).wait_recv()
        value = own[k] + mix(k, 2 * twin, f1[k, twin])
        partial[k, twin] = cube(value)
        ex2(k, twin).start()
        first[k] = value
    for side in range(2):
        ex_m(side, 0).start()

    for k in range(LEV):
        ex1(k, remote_side).wait_recv()
        part = mix(k, 2 * remote_side, f1[k, remote_side])
        partial[k, remote_side] = cube(own[k] + part)
        ex2(k, remote_side).start()
        value = first[k] + part
        first[k] = value
        base[k] = mix(k, 1, value) + src[k].reshape(PTS, Q)

        @pl.when(edge)
        def _():
            if k >= 1:
                second_from(k - 1, near, True)
            if k == 1:
                matrix_in(near, 0)
            if k == 2:
                take(0, near)
                correct_once(0, near)
            if k >= 2:
                take(k - 1, near)
                correct_once(k - 1, near)
                relay(k - 2, near)

    @pl.when(edge)
    def _():
        second_from(LEV - 1, near, True)
        take(LEV - 1, near)
        correct_once(LEV - 1, near)
        for k in (LEV - 2, LEV - 1):
            relay(k, near)
        for side in range(2):
            ex_m(side, 1).start()

    meet(remote_side)

    @pl.when(jnp.logical_not(edge))
    def _():
        for k in range(LEV):
            second_from(k, ahead, True)
        for k in range(LEV):
            second_from(k, 1 - ahead, False)
        for k in range(LEV):
            take(k, near)
            take(k, far)
        matrix_in(near, 0)
        for k in range(LEV):
            correct_once(k, near)
            relay(k, near)
        for side in range(2):
            ex_m(side, 1).start()

    @pl.when(edge)
    def _():
        for k in range(LEV):
            second_from(k, far, False)
            take(k, far)

    matrix_in(far, 0)
    for k in range(LEV):
        correct_once(k, far)
    for k in range(LEV - 1):
        relay(k, far)
    through = jnp.concatenate(
        [dot3(sn_hi[side, 0], sn_lo[side, 0], back_hi[side], back_lo[side]) for side in range(2)], axis=0
    )
    h = jnp.where(unit, 1.0, 0.0) - VISCOSITY * (gg + dot_split(r_out, through))
    hi, lo = split(h)
    h_hi[...] = hi
    h_lo[...] = lo

    relay(LEV - 1, far)
    for k in range(LEV):
        settle(k)
    correct_twice(near)

    def gather(k, whole):
        wait_bytes(twice_in.at[k], recvq.at[k])
        for side in range(2):
            terms_in[k, side, pl.ds(64, 64)] = twice_in[k, side] + jnp.where(
                whole | (side == near), corr[k, side, pl.ds(64, 64)], 0.0
            )
        hi, lo = split(terms_in[k].reshape(PTS, Q))
        return total[k] + dot3(e_hi[...], e_lo[...], hi, lo)

    @pl.when(edge)
    def _():
        for k in range(LEV):
            total[k] = gather(k, False)
        correct_twice(far)
        for k in range(LEV):
            hi, lo = split(corr[k, far, pl.ds(64, 64)])
            outbuf[:, k] = cube(total[k] + dot3(eq_hi[far], eq_lo[far], hi, lo))

    @pl.when(jnp.logical_not(edge))
    def _():
        correct_twice(far)
        for k in range(LEV):
            outbuf[:, k] = cube(gather(k, True))

    for side in range(2):
        wait_bytes(span, sent.at[side])


def local(tracers, sources, weights, dep_owner, dep_slot, nbr_elem, nbr_edge, metric):
    count = lax.axis_size("elem")
    block = (LEV, 16, 16, Q)
    dma = pltpu.SemaphoreType.DMA
    vmem = pltpu.VMEM
    pairs = (LEV, 2, 16, 16, Q)
    flat = (LEV, PTS, Q)
    tall = (2, 128, PTS)
    slim = (LEV, 2, 64, Q)
    scratch = [
        vmem(block, F32), vmem(block, F32), vmem((16, LEV, 384), F32),
        vmem(dep_owner.shape, I32), vmem(dep_slot.shape, I32),
        vmem(nbr_elem.shape[::-1], I32), vmem(nbr_edge.shape[::-1], I32), vmem(metric.shape, F32),
        vmem(pairs, F32), vmem(flat, F32), vmem(pairs, F32), vmem(flat, F32),
        vmem(pairs, F32), vmem((LEV, 2, PTS, Q), F32), vmem(flat, F32), vmem(flat, F32),
        vmem((LEV, 3, PTS, PTS), BF16), vmem((LEV, 3, PTS, PTS), BF16),
        vmem((2, 16, LEV, 384), F32), vmem((LEV, 2, PTS, PTS), BF16), vmem((LEV, 2, PTS, PTS), BF16),
        vmem((LEV, 2, PTS, Q), BF16), vmem((LEV, 2, PTS, Q), BF16), vmem((47, 64, 128), F32),
        vmem(tall, F32), vmem(tall, BF16), vmem(tall, BF16),
        vmem(tall, F32), vmem((2, 2, 64, PTS), BF16), vmem((2, 2, 64, PTS), BF16),
        vmem((LEV, 2, 128, Q), F32), vmem((2, 64, 64), BF16), vmem((2, 64, 64), BF16),
        vmem(slim, F32), vmem(slim, F32), vmem(slim, F32), vmem(slim, F32), vmem(slim, F32),
        vmem((LEV, 2, 128, Q), F32),
        vmem((PTS, PTS), BF16), vmem((PTS, PTS), BF16),
        vmem((PTS, PTS), BF16), vmem((PTS, PTS), BF16),
        vmem((2, PTS, 64), BF16), vmem((2, PTS, 64), BF16),
        vmem((2, PTS, PTS), BF16), vmem((2, PTS, PTS), BF16),
        dma((6,)), dma((2,)),
        dma((2,)), dma((LEV, 2)), dma((LEV, 2)), dma((3, 2)), dma((LEV, 2)), dma((LEV,)),
    ]
    return pl.pallas_call(
        functools.partial(kernel, count),
        out_shape=pltpu.VMEM(tracers.shape, F32),
        in_specs=[pl.BlockSpec(memory_space=pl.ANY)] * 8,
        out_specs=pl.BlockSpec(memory_space=pltpu.VMEM),
        scratch_shapes=scratch,
        compiler_params=pltpu.CompilerParams(collective_id=0, has_side_effects=True),
        name="tracer_step",
    )(tracers, sources, weights, dep_owner, dep_slot, nbr_elem.T, nbr_edge.T, metric)


def solution(mesh):
    placed = (
        P("elem", None, None, None),
        P("elem", None, None, None),
        P("elem", None, None),
        P("elem", None, None),
        P("elem", None, None),
        P("elem", None),
        P("elem", None),
        P("elem", None, None),
    )
    return jax.shard_map(
        local, mesh=mesh, in_specs=placed, out_specs=P("elem", None, None, None), check_vma=False
    )
```

```python
import functools

import jax
import jax.numpy as jnp
import numpy as np
from jax import lax
from jax.experimental import pallas as pl
from jax.experimental.pallas import tpu as pltpu
from jax.sharding import PartitionSpec as P

VISCOSITY = 0.002
LEV = 4
PTS = 256
Q = 128
F32 = jnp.float32
BF16 = jnp.bfloat16
I32 = jnp.int32


def derivative_matrix():
    nodes = np.array([-1.0, -np.sqrt(0.2), np.sqrt(0.2), 1.0])
    count = nodes.shape[0]
    bary = np.array(
        [1.0 / np.prod([nodes[j] - nodes[m] for m in range(count) if m != j]) for j in range(count)]
    )
    derivative = np.zeros((count, count))
    for i in range(count):
        for j in range(count):
            if i != j:
                derivative[i, j] = bary[j] / bary[i] / (nodes[i] - nodes[j])
        derivative[i, i] = -np.sum(derivative[i])
    return derivative


def rows(shape):
    return lax.broadcasted_iota(I32, shape, 0)


def cols(shape):
    return lax.broadcasted_iota(I32, shape, 1)


def dot(a, b):
    return jnp.dot(a, b, preferred_element_type=F32)


def split(x):
    hi = x.astype(BF16)
    lo = (x - hi.astype(F32)).astype(BF16)
    return hi, lo


def dot3(a_hi, a_lo, b_hi, b_lo):
    n = b_hi.shape[1]
    both = dot(a_hi, jnp.concatenate([b_hi, b_lo], axis=1))
    return both[:, :n] + (both[:, n:] + dot(a_lo, b_hi))


def dot_split(a, b):
    return dot3(*split(a), *split(b))


def edge_point(s, k):
    return jnp.where(s == 0, 4 * k, jnp.where(s == 1, 12 + k, jnp.where(s == 2, 15 - 4 * k, 3 - k)))


def direction_table(shape, along_b):
    m, p = rows(shape) & 15, cols(shape) & 15
    if along_b:
        i, j, live = m & 3, p & 3, (m >> 2) == (p >> 2)
    else:
        i, j, live = m >> 2, p >> 2, (m & 3) == (p & 3)
    which = jnp.where(live, i * 4 + j, -1)
    table = derivative_matrix()
    value = jnp.zeros(shape, F32)
    for at in range(16):
        value = jnp.where(which == at, np.float32(table[at // 4, at % 4]), value)
    return value


def offset_of(owner, me, count):
    d = owner - me
    d = jnp.where(d > 1, d - count, d)
    d = jnp.where(d < -1, d + count, d)
    return d + 1


def kernel(
    count,
    tracers, sources, weights, dep_owner, dep_slot, nbr_elem, nbr_edge, metric,
    outbuf,
    own_t, src, wx, cd, cd_in, dow, dsl, nel, ned, met,
    f1, own, partial, first, f2, fix, base, total,
    w_hi, w_lo, wx_in, nb_hi, nb_lo, taken_hi, taken_lo, span,
    km_cut, km_in, km_twice, km_twice_in, mine, sm_hi, sm_lo, sn_hi, sn_lo,
    corr, vz_hi, vz_lo, once, twice_own, twice, once_in, twice_in, terms_in,
    h_hi, h_lo, e_hi, e_lo, back_hi, back_lo,
    loc, loc_t,
    sent, recv1, recv2, recvm, recvp, recvq,
):
    me = lax.axis_index("elem")
    place_in_row = lax.rem(me, 8)
    near = jnp.where(place_in_row < 4, 1, 0)
    far = 1 - near
    edge = (place_in_row == 0) | (place_in_row == 7)
    twin = jnp.where(lax.rem(me, 2) == 0, 1, 0)
    remote_side = 1 - twin
    middle = (place_in_row == 3) | (place_in_row == 4)
    ahead = jnp.where(middle, far, near)

    def beyond(side):
        return lax.rem(me + 1 - 2 * side + count, count)

    def remote(source, target, send_sem, recv_sem, side):
        return pltpu.make_async_remote_copy(
            src_ref=source,
            dst_ref=target,
            send_sem=send_sem,
            recv_sem=recv_sem,
            device_id=(beyond(side),),
            device_id_type=pl.DeviceIdType.MESH,
        )

    small = [
        pltpu.make_async_copy(a, b, loc.at[i])
        for i, (a, b) in enumerate(
            [
                (weights, wx),
                (dep_owner, dow),
                (dep_slot, dsl),
                (nbr_elem, nel),
                (nbr_edge, ned),
                (metric, met),
            ]
        )
    ]
    load_t = [pltpu.make_async_copy(tracers.at[:, k], own_t.at[k], loc_t.at[1 + k]) for k in range(LEV)]
    load_s = [pltpu.make_async_copy(sources.at[:, k], src.at[k], loc_t.at[0]) for k in range(LEV)]

    def wait_bytes(like, semaphore):
        pltpu.make_async_copy(like, like, semaphore).wait()

    def ex1(k, side):
        return remote(own_t.at[k], f1.at[k, side], sent.at[side], recv1.at[k, side], side)

    def ex2(k, side):
        return remote(partial.at[k, side], f2.at[k, side], sent.at[side], recv2.at[k, side], side)

    def ex_w(side):
        return remote(wx, wx_in.at[side], sent.at[side], recvm.at[0, side], side)

    def ex_c(side):
        return remote(cd, cd_in.at[side], sent.at[side], recvm.at[3, side], side)

    def ex_m(side, part):
        ends = ((km_cut, km_in), (km_twice, km_twice_in))[part]
        return remote(
            ends[0].at[side], ends[1].at[side], sent.at[side], recvm.at[1 + part, side], side
        )

    def ex_p(k, side):
        return remote(once.at[k, side], once_in.at[k, side], sent.at[side], recvp.at[k, side], side)

    def ex_q(k, side):
        return remote(twice.at[k, side], twice_in.at[k, side], sent.at[side], recvq.at[k], side)

    barrier = pltpu.get_barrier_semaphore()
    for side in range(2):
        pl.semaphore_signal(
            barrier, inc=1, device_id=(beyond(side),), device_id_type=pl.DeviceIdType.MESH
        )
    for c in load_t:
        c.start()
    for c in small:
        c.start()
    for c in load_s:
        c.start()
    pl.semaphore_wait(barrier, 2)
    for k in range(LEV):
        load_t[k].wait()
        for side in range(2):
            ex1(k, side).start()

    for c in small:
        c.wait()
    cd[...] = jnp.zeros((16, 128), F32)
    for e in range(16):
        code = (offset_of(dow[e], me, count) * 16 + dsl[e]).astype(F32)
        for k in range(LEV):
            cd[pl.ds(e, 1), pl.ds(16 * k, 16)] = code[k : k + 1]
    for side in range(2):
        ex_w(side).start()
        ex_c(side).start()
    wait_bytes(src, loc_t.at[0])
    diagonal = (cols((16, PTS)) >> 4) == rows((16, PTS))
    eye16 = cols((16, 16)) == rows((16, 16))
    tile_j = ((rows((PTS, PTS)) & 15) == (cols((PTS, PTS)) & 15)).astype(F32).astype(BF16)
    lane_elem = (cols((1, PTS)) >> 4).astype(F32)

    def tiled(table, marks, k):
        his, los, codes = [], [], []
        for e in range(16):
            row = table[e, pl.ds(k, 1), :]
            hi = row.astype(BF16).astype(F32)
            his.append(jnp.where(diagonal, jnp.broadcast_to(hi, (16, PTS)), 0.0))
            los.append(jnp.where(diagonal, jnp.broadcast_to(row - hi, (16, PTS)), 0.0))
            code = marks[pl.ds(e, 1), pl.ds(16 * k, 16)]
            codes.append(jnp.where(eye16, jnp.broadcast_to(code, (16, 16)), 0.0))
        hi = dot(jnp.concatenate(his, axis=0).astype(BF16), tile_j)
        lo = dot(jnp.concatenate(los, axis=0).astype(BF16), tile_j)
        code = jnp.sum(jnp.concatenate(codes, axis=0), axis=1, keepdims=True)
        return hi, lo, code

    def mix(k, i, field):
        hi, lo = split(field.reshape(PTS, Q))
        return dot3(w_hi[k, i], w_lo[k, i], hi, lo)

    def cube(x):
        return x.reshape(16, 16, Q)

    for k in range(LEV):
        hi, lo, code = tiled(wx, cd, k)
        for i in range(3):
            match = code == (lane_elem + float(16 * i))
            w_hi[k, i] = jnp.where(match, hi, 0.0).astype(BF16)
            w_lo[k, i] = jnp.where(match, lo, 0.0).astype(BF16)
        own[k] = mix(k, 1, own_t[k]) + src[k].reshape(PTS, Q)

    square = (PTS, PTS)
    r, c = rows(square), cols(square)
    same_elem = (r >> 4) == (c >> 4)
    unit = r == c
    left_a, left_b = direction_table((16, 16), False), direction_table((16, 16), True)
    right_a, right_b = direction_table((16, PTS), False), direction_table((16, PTS), True)
    fa, fb = [], []
    for e in range(16):
        fa.append(left_a * jnp.broadcast_to(met[e, pl.ds(0, 1), :], (16, 16)))
        fb.append(left_b * jnp.broadcast_to(met[e, pl.ds(1, 1), :], (16, 16)))
    full = dot_split(jnp.concatenate(fa, axis=0), right_a) + dot_split(jnp.concatenate(fb, axis=0), right_b)
    m = jnp.where(same_elem, full, 0.0)

    edge_row, edge_col = rows((PTS, 16)), cols((PTS, 16))

    def edge_column(table):
        spread_out = jnp.zeros((PTS, 16), F32)
        for s in range(4):
            here = ((edge_row >> 4) == edge_col) & (((edge_row >> 2) & 3) == s)
            line = table[pl.ds(s, 1), :].astype(F32)
            spread_out = jnp.where(here, jnp.broadcast_to(line, (PTS, 16)), spread_out)
        return jnp.sum(spread_out, axis=1, keepdims=True).astype(I32)

    ne, nt = edge_column(nel), edge_column(ned)
    off = offset_of(ne >> 4, me, count)
    pe = (ne & 15) * 4 + nt
    off_f, pe_f = off.astype(F32), pe.astype(F32)
    off_row = jnp.sum(jnp.where(unit, off_f, 0.0), axis=0, keepdims=True)
    pe_row = jnp.sum(jnp.where(unit, pe_f, 0.0), axis=0, keepdims=True)
    peer = (off_row == off_f) & ((c & 3) == 0)
    rank_own = jnp.sum(jnp.where(peer & ((c >> 2) < (r >> 2)), 1.0, 0.0), axis=1, keepdims=True).astype(I32)
    rank_pe = jnp.sum(jnp.where(peer & (pe_row < pe_f), 1.0, 0.0), axis=1, keepdims=True).astype(I32)
    point = rows((PTS, 1)) & 3
    slot = jnp.where(off == 1, pe, jnp.where(off == 0, 64 + rank_pe, 80 + rank_pe))
    take = (cols((PTS, 384)) == slot * 4 + 3 - point).astype(F32).astype(BF16)
    place = jnp.where(off == 1, -1, jnp.where(off == 2, 0, 64) + rank_own * 4 + point)
    pack_t = (cols((PTS, 128)) == place).astype(F32)
    pack = pack_t.T.astype(BF16)
    spread_t = (same_elem & ((r & 15) == edge_point((c >> 2) & 3, c & 3))).astype(F32).astype(BF16)
    spread = (same_elem & ((c & 15) == edge_point((r >> 2) & 3, r & 3))).astype(F32).astype(BF16)
    a, b = (rows((PTS, 1)) >> 2) & 3, rows((PTS, 1)) & 3
    rim_a, rim_b = ((a == 0) | (a == 3)).astype(F32), ((b == 0) | (b == 3)).astype(F32)
    counts = 1.0 + rim_a + rim_b
    added = dot(spread_t, take)
    own_add = dot(added[:, :PTS].astype(BF16), spread)
    r_own = (jnp.where(unit, 1.0, 0.0) + own_add) / counts
    r_out = added[:, PTS:] / counts
    picked = dot(pack, spread)
    km = dot_split(picked, m)
    g = dot_split(r_own, m)
    for side, through in enumerate((dot_split(km[:64], r_out[:, :64]), dot_split(km[64:], r_out[:, 64:]))):
        hi, lo = split(through)
        vz_hi[side] = hi
        vz_lo[side] = lo
    lands = ((off != 1) & (c == pe * 4 + 3 - point)).astype(F32).astype(BF16)
    landed = dot(pack, lands).T.astype(BF16)
    r_nb = dot(spread_t, landed) / counts
    for side, back in enumerate((dot_split(r_nb[:, 64:], km[64:]), dot_split(r_nb[:, :64], km[:64]))):
        hi, lo = split(back)
        back_hi[side] = hi
        back_lo[side] = lo
    kmg = dot_split(km, g)
    fold = ((rows((PTS, 128)) & 15) == cols((PTS, 128))).astype(F32)
    cut = dot_split(km, fold)
    for side in range(2):
        km_cut[side] = cut[64 * side : 64 * side + 64]
        km_twice[side] = kmg[64 * side : 64 * side + 64]
    unfold = (rows((128, PTS)) == (cols((128, PTS)) & 15)).astype(F32).astype(BF16)
    place_pe = jnp.where(off == 1, -1, jnp.where(off == 2, 0, 64) + rank_pe * 4 + point)
    arrive = (cols((PTS, 128)) == place_pe).astype(F32).T.astype(BF16)
    facing = dot(dot(arrive, lands).astype(BF16), same_elem.astype(F32).astype(BF16))
    mine[1] = (facing[:64] > 0.5).astype(F32)
    mine[0] = (facing[64:] > 0.5).astype(F32)
    for side in range(2):
        hi, lo = split(
            jnp.concatenate(
                [km[64 * side : 64 * side + 64], kmg[64 * side : 64 * side + 64]], axis=0
            )
        )
        sm_hi[side] = hi
        sm_lo[side] = lo
    gr = dot_split(g, r_out)
    gg = dot_split(g, g)
    ext = -VISCOSITY * jnp.concatenate([gr[:, :64], r_out[:, :64], gr[:, 64:], r_out[:, 64:]], axis=1)
    hi, lo = split(ext)
    e_hi[...] = hi
    e_lo[...] = lo

    def meet(side):
        ex_w(side).wait_recv()
        ex_c(side).wait_recv()
        shift = jnp.where(side == 0, 32.0, 0.0)
        for k in range(LEV):
            hi, lo, code = tiled(wx_in.at[side], cd_in.at[side], k)
            match = code == (lane_elem + shift)
            n_hi = jnp.where(match, hi, 0.0).astype(BF16)
            n_lo = jnp.where(match, lo, 0.0).astype(BF16)
            nb_hi[k, side] = n_hi
            nb_lo[k, side] = n_lo
            hi, lo = split(own_t[k].reshape(PTS, Q))
            fix[k, side] = dot3(n_hi, n_lo, hi, lo)

    def matrix_in(side, part):
        ex_m(side, part).wait_recv()
        if part == 0:
            hi, lo = split(km_in[side])
            hi, lo = split((dot(hi, unfold) + dot(lo, unfold)) * mine[side])
        else:
            hi, lo = split(km_twice_in[side])
        sn_hi[side, part] = hi
        sn_lo[side, part] = lo

    def take(k, side):
        hi, lo = split(first[k])
        hi, lo = split(dot3(nb_hi[k, side], nb_lo[k, side], hi, lo))
        taken_hi[k, side] = hi
        taken_lo[k, side] = lo

    def correct_once(k, side):
        corr[k, side, pl.ds(0, 64)] = dot3(
            sn_hi[side, 0], sn_lo[side, 0], taken_hi[k, side], taken_lo[k, side]
        )

    def correct_twice(side):
        matrix_in(side, 1)
        for k in range(LEV):
            corr[k, side, pl.ds(64, 64)] = dot3(
                sn_hi[side, 1], sn_lo[side, 1], taken_hi[k, side], taken_lo[k, side]
            )

    def second_from(k, side, start):
        ex2(k, side).wait_recv()
        part = mix(k, 2 * side, f2[k, side].reshape(PTS, Q) + fix[k, side])
        here = base[k]
        hi, lo = split(here + part)
        terms = dot3(sm_hi[side], sm_lo[side], hi, lo)
        once[k, side] = terms[:64]
        twice_own[k, side] = terms[64:]
        ex_p(k, side).start()
        total[k] = (here if start else total[k]) + part

    def settle(k):
        hi, lo = split(total[k])
        total[k] = dot3(h_hi[...], h_lo[...], hi, lo)

    def relay(k, side):
        ex_p(k, side).wait_recv()
        whole = once_in[k, side] + corr[k, side, pl.ds(0, 64)]
        terms_in[k, side, pl.ds(0, 64)] = whole
        hi, lo = split(whole)
        twice[k, side] = twice_own[k, side] + dot3(vz_hi[side], vz_lo[side], hi, lo)
        ex_q(k, side).start()

    meet(twin)
    for k in range(LEV):
        ex1(k, twin).wait_recv()
        value = own[k] + mix(k, 2 * twin, f1[k, twin])
        partial[k, twin] = cube(value)
        ex2(k, twin).start()
        first[k] = value
    for part in range(2):
        for side in range(2):
            ex_m(side, part).start()

    for k in range(LEV):
        ex1(k, remote_side).wait_recv()
        part = mix(k, 2 * remote_side, f1[k, remote_side])
        partial[k, remote_side] = cube(own[k] + part)
        ex2(k, remote_side).start()
        value = first[k] + part
        first[k] = value
        base[k] = mix(k, 1, value) + src[k].reshape(PTS, Q)

        @pl.when(edge)
        def _():
            second_from(k, near, True)
            if k == 1:
                matrix_in(near, 0)
            if k >= 1:
                take(k - 1, near)
                correct_once(k - 1, near)

    @pl.when(edge)
    def _():
        take(LEV - 1, near)
        correct_once(LEV - 1, near)
        for k in range(LEV):
            relay(k, near)

    meet(remote_side)

    @pl.when(jnp.logical_not(edge))
    def _():
        for k in range(LEV):
            second_from(k, ahead, True)
        for k in range(LEV):
            second_from(k, 1 - ahead, False)
        for k in range(LEV):
            take(k, near)
            take(k, far)
        matrix_in(near, 0)
        for k in range(LEV):
            correct_once(k, near)
            relay(k, near)

    @pl.when(edge)
    def _():
        for k in range(LEV):
            second_from(k, far, False)
            take(k, far)

    matrix_in(far, 0)
    for k in range(LEV):
        correct_once(k, far)
    for k in range(LEV - 1):
        relay(k, far)
    through = jnp.concatenate(
        [dot3(sn_hi[side, 0], sn_lo[side, 0], back_hi[side], back_lo[side]) for side in range(2)], axis=0
    )
    h = jnp.where(unit, 1.0, 0.0) - VISCOSITY * (gg + dot_split(r_out, through))
    hi, lo = split(h)
    h_hi[...] = hi
    h_lo[...] = lo

    relay(LEV - 1, far)
    for k in range(LEV):
        settle(k)
    correct_twice(near)

    correct_twice(far)
    for k in range(LEV):
        wait_bytes(twice_in.at[k], recvq.at[k])
        for side in range(2):
            terms_in[k, side, pl.ds(64, 64)] = twice_in[k, side] + corr[k, side, pl.ds(64, 64)]
        hi, lo = split(terms_in[k].reshape(PTS, Q))
        outbuf[:, k] = cube(total[k] + dot3(e_hi[...], e_lo[...], hi, lo))

    for side in range(2):
        wait_bytes(span, sent.at[side])


def local(tracers, sources, weights, dep_owner, dep_slot, nbr_elem, nbr_edge, metric):
    count = lax.axis_size("elem")
    block = (LEV, 16, 16, Q)
    dma = pltpu.SemaphoreType.DMA
    vmem = pltpu.VMEM
    pairs = (LEV, 2, 16, 16, Q)
    flat = (LEV, PTS, Q)
    tall = (2, 128, PTS)
    slim = (LEV, 2, 64, Q)
    scratch = [
        vmem(block, F32), vmem(block, F32), vmem((16, LEV, PTS), F32), vmem((16, 128), F32),
        vmem((2, 16, 128), F32), vmem(dep_owner.shape, I32), vmem(dep_slot.shape, I32),
        vmem(nbr_elem.shape[::-1], I32), vmem(nbr_edge.shape[::-1], I32), vmem(metric.shape, F32),
        vmem(pairs, F32), vmem(flat, F32), vmem(pairs, F32), vmem(flat, F32),
        vmem(pairs, F32), vmem((LEV, 2, PTS, Q), F32), vmem(flat, F32), vmem(flat, F32),
        vmem((LEV, 3, PTS, PTS), BF16), vmem((LEV, 3, PTS, PTS), BF16),
        vmem((2, 16, LEV, PTS), F32), vmem((LEV, 2, PTS, PTS), BF16), vmem((LEV, 2, PTS, PTS), BF16),
        vmem((LEV, 2, PTS, Q), BF16), vmem((LEV, 2, PTS, Q), BF16), vmem((181, 16, 128), F32),
        vmem((2, 64, 128), F32), vmem((2, 64, 128), F32), vmem((2, 64, PTS), F32),
        vmem((2, 64, PTS), F32), vmem((2, 64, PTS), F32), vmem(tall, BF16), vmem(tall, BF16),
        vmem((2, 2, 64, PTS), BF16), vmem((2, 2, 64, PTS), BF16),
        vmem((LEV, 2, 128, Q), F32), vmem((2, 64, 64), BF16), vmem((2, 64, 64), BF16),
        vmem(slim, F32), vmem(slim, F32), vmem(slim, F32), vmem(slim, F32), vmem(slim, F32),
        vmem((LEV, 2, 128, Q), F32),
        vmem((PTS, PTS), BF16), vmem((PTS, PTS), BF16),
        vmem((PTS, PTS), BF16), vmem((PTS, PTS), BF16),
        vmem((2, PTS, PTS), BF16), vmem((2, PTS, PTS), BF16),
        dma((6,)), dma((1 + LEV,)),
        dma((2,)), dma((LEV, 2)), dma((LEV, 2)), dma((4, 2)), dma((LEV, 2)), dma((LEV,)),
    ]
    return pl.pallas_call(
        functools.partial(kernel, count),
        out_shape=pltpu.VMEM(tracers.shape, F32),
        in_specs=[pl.BlockSpec(memory_space=pl.ANY)] * 8,
        out_specs=pl.BlockSpec(memory_space=pltpu.VMEM),
        scratch_shapes=scratch,
        compiler_params=pltpu.CompilerParams(collective_id=0, has_side_effects=True),
        name="tracer_step",
    )(tracers, sources, weights, dep_owner, dep_slot, nbr_elem.T, nbr_edge.T, metric)


def solution(mesh):
    placed = (
        P("elem", None, None, None),
        P("elem", None, None, None),
        P("elem", None, None),
        P("elem", None, None),
        P("elem", None, None),
        P("elem", None),
        P("elem", None),
        P("elem", None, None),
    )
    return jax.shard_map(
        local, mesh=mesh, in_specs=placed, out_specs=P("elem", None, None, None), check_vma=False
    )
```

```python
import functools

import jax
import jax.numpy as jnp
import numpy as np
from jax import lax
from jax.experimental import pallas as pl
from jax.experimental.pallas import tpu as pltpu
from jax.sharding import PartitionSpec as P

VISCOSITY = 0.002
LEV = 4
PTS = 256
Q = 128
F32 = jnp.float32
BF16 = jnp.bfloat16
I32 = jnp.int32


def derivative_matrix():
    nodes = np.array([-1.0, -np.sqrt(0.2), np.sqrt(0.2), 1.0])
    count = nodes.shape[0]
    bary = np.array(
        [1.0 / np.prod([nodes[j] - nodes[m] for m in range(count) if m != j]) for j in range(count)]
    )
    derivative = np.zeros((count, count))
    for i in range(count):
        for j in range(count):
            if i != j:
                derivative[i, j] = bary[j] / bary[i] / (nodes[i] - nodes[j])
        derivative[i, i] = -np.sum(derivative[i])
    return derivative


def rows(shape):
    return lax.broadcasted_iota(I32, shape, 0)


def cols(shape):
    return lax.broadcasted_iota(I32, shape, 1)


def dot(a, b):
    return jnp.dot(a, b, preferred_element_type=F32)


def split(x):
    hi = x.astype(BF16)
    lo = (x - hi.astype(F32)).astype(BF16)
    return hi, lo


def dot3(a_hi, a_lo, b_hi, b_lo):
    n = b_hi.shape[1]
    both = dot(a_hi, jnp.concatenate([b_hi, b_lo], axis=1))
    return both[:, :n] + (both[:, n:] + dot(a_lo, b_hi))


def dot_split(a, b):
    return dot3(*split(a), *split(b))


def edge_point(s, k):
    return jnp.where(s == 0, 4 * k, jnp.where(s == 1, 12 + k, jnp.where(s == 2, 15 - 4 * k, 3 - k)))


def direction_table(shape, along_b):
    m, p = rows(shape) & 15, cols(shape) & 15
    if along_b:
        i, j, live = m & 3, p & 3, (m >> 2) == (p >> 2)
    else:
        i, j, live = m >> 2, p >> 2, (m & 3) == (p & 3)
    which = jnp.where(live, i * 4 + j, -1)
    table = derivative_matrix()
    value = jnp.zeros(shape, F32)
    for at in range(16):
        value = jnp.where(which == at, np.float32(table[at // 4, at % 4]), value)
    return value


def offset_of(owner, me, count):
    d = owner - me
    d = jnp.where(d > 1, d - count, d)
    d = jnp.where(d < -1, d + count, d)
    return d + 1


def kernel(
    count,
    tracers, sources, weights, dep_owner, dep_slot, nbr_elem, nbr_edge, metric,
    outbuf,
    own_t, src, wx, cd, cd_in, dow, dsl, nel, ned, met,
    f1, own, partial, first, f2, fix, base, total,
    w_hi, w_lo, wx_in, nb_hi, nb_lo, taken_hi, taken_lo, span,
    km_cut, km_in, km_twice, km_twice_in, mine, sm_hi, sm_lo, sn_hi, sn_lo,
    corr, vz_hi, vz_lo, once, twice_own, twice, once_in, twice_in, terms_in,
    h_hi, h_lo, e_hi, e_lo, back_hi, back_lo,
    loc, loc_t,
    sent, recv1, recv2, recvm, recvp, recvq,
):
    me = lax.axis_index("elem")
    place_in_row = lax.rem(me, 8)
    near = jnp.where(place_in_row < 4, 1, 0)
    far = 1 - near
    edge = (place_in_row == 0) | (place_in_row == 7)
    twin = jnp.where(lax.rem(me, 2) == 0, 1, 0)
    remote_side = 1 - twin
    middle = (place_in_row == 3) | (place_in_row == 4)
    ahead = jnp.where(middle, far, near)

    def beyond(side):
        return lax.rem(me + 1 - 2 * side + count, count)

    def remote(source, target, send_sem, recv_sem, side):
        return pltpu.make_async_remote_copy(
            src_ref=source,
            dst_ref=target,
            send_sem=send_sem,
            recv_sem=recv_sem,
            device_id=(beyond(side),),
            device_id_type=pl.DeviceIdType.MESH,
        )

    small = [
        pltpu.make_async_copy(a, b, loc.at[i])
        for i, (a, b) in enumerate(
            [
                (weights, wx),
                (dep_owner, dow),
                (dep_slot, dsl),
                (nbr_elem, nel),
                (nbr_edge, ned),
                (metric, met),
            ]
        )
    ]
    load_t = [pltpu.make_async_copy(tracers.at[:, k], own_t.at[k], loc_t.at[1 + k]) for k in range(LEV)]
    load_s = [pltpu.make_async_copy(sources.at[:, k], src.at[k], loc_t.at[0]) for k in range(LEV)]

    def wait_bytes(like, semaphore):
        pltpu.make_async_copy(like, like, semaphore).wait()

    def ex1(k, side):
        return remote(own_t.at[k], f1.at[k, side], sent.at[side], recv1.at[k, side], side)

    def ex2(k, side):
        return remote(partial.at[k, side], f2.at[k, side], sent.at[side], recv2.at[k, side], side)

    def ex_w(side):
        return remote(wx, wx_in.at[side], sent.at[side], recvm.at[0, side], side)

    def ex_c(side):
        return remote(cd, cd_in.at[side], sent.at[side], recvm.at[3, side], side)

    def ex_m(side, part):
        ends = ((km_cut, km_in), (km_twice, km_twice_in))[part]
        return remote(
            ends[0].at[side], ends[1].at[side], sent.at[side], recvm.at[1 + part, side], side
        )

    def ex_p(k, side):
        return remote(once.at[k, side], once_in.at[k, side], sent.at[side], recvp.at[k, side], side)

    def ex_q(k, side):
        return remote(twice.at[k, side], twice_in.at[k, side], sent.at[side], recvq.at[k], side)

    barrier = pltpu.get_barrier_semaphore()
    for side in range(2):
        pl.semaphore_signal(
            barrier, inc=1, device_id=(beyond(side),), device_id_type=pl.DeviceIdType.MESH
        )
    for c in load_t:
        c.start()
    for c in small:
        c.start()
    for c in load_s:
        c.start()

    def send_tracers(loaded):
        pl.semaphore_wait(barrier, 2)
        for k in range(LEV):
            if not loaded:
                load_t[k].wait()
            for side in range(2):
                ex1(k, side).start()

    def send_tables():
        for side in range(2):
            ex_w(side).start()
            ex_c(side).start()

    first_of_all = me == 0
    others = jnp.logical_not(first_of_all)

    @pl.when(others)
    def _():
        send_tracers(False)

    @pl.when(first_of_all)
    def _():
        for k in range(LEV):
            load_t[k].wait()

    for c in small:
        c.wait()
    cd[...] = jnp.zeros((16, 128), F32)
    for e in range(16):
        code = (offset_of(dow[e], me, count) * 16 + dsl[e]).astype(F32)
        for k in range(LEV):
            cd[pl.ds(e, 1), pl.ds(16 * k, 16)] = code[k : k + 1]
    pl.when(others)(send_tables)
    wait_bytes(src, loc_t.at[0])
    diagonal = (cols((16, PTS)) >> 4) == rows((16, PTS))
    eye16 = cols((16, 16)) == rows((16, 16))
    tile_j = ((rows((PTS, PTS)) & 15) == (cols((PTS, PTS)) & 15)).astype(F32).astype(BF16)
    lane_elem = (cols((1, PTS)) >> 4).astype(F32)

    def tiled(table, marks, k):
        his, los, codes = [], [], []
        for e in range(16):
            row = table[e, pl.ds(k, 1), :]
            hi = row.astype(BF16).astype(F32)
            his.append(jnp.where(diagonal, jnp.broadcast_to(hi, (16, PTS)), 0.0))
            los.append(jnp.where(diagonal, jnp.broadcast_to(row - hi, (16, PTS)), 0.0))
            code = marks[pl.ds(e, 1), pl.ds(16 * k, 16)]
            codes.append(jnp.where(eye16, jnp.broadcast_to(code, (16, 16)), 0.0))
        hi = dot(jnp.concatenate(his, axis=0).astype(BF16), tile_j)
        lo = dot(jnp.concatenate(los, axis=0).astype(BF16), tile_j)
        code = jnp.sum(jnp.concatenate(codes, axis=0), axis=1, keepdims=True)
        return hi, lo, code

    def mix(k, i, field):
        hi, lo = split(field.reshape(PTS, Q))
        return dot3(w_hi[k, i], w_lo[k, i], hi, lo)

    def cube(x):
        return x.reshape(16, 16, Q)

    for k in range(LEV):
        hi, lo, code = tiled(wx, cd, k)
        for i in range(3):
            match = code == (lane_elem + float(16 * i))
            w_hi[k, i] = jnp.where(match, hi, 0.0).astype(BF16)
            w_lo[k, i] = jnp.where(match, lo, 0.0).astype(BF16)
        own[k] = mix(k, 1, own_t[k]) + src[k].reshape(PTS, Q)

    square = (PTS, PTS)
    r, c = rows(square), cols(square)
    same_elem = (r >> 4) == (c >> 4)
    unit = r == c
    left_a, left_b = direction_table((16, 16), False), direction_table((16, 16), True)
    right_a, right_b = direction_table((16, PTS), False), direction_table((16, PTS), True)
    fa, fb = [], []
    for e in range(16):
        fa.append(left_a * jnp.broadcast_to(met[e, pl.ds(0, 1), :], (16, 16)))
        fb.append(left_b * jnp.broadcast_to(met[e, pl.ds(1, 1), :], (16, 16)))
    full = dot_split(jnp.concatenate(fa, axis=0), right_a) + dot_split(jnp.concatenate(fb, axis=0), right_b)
    m = jnp.where(same_elem, full, 0.0)

    edge_row, edge_col = rows((PTS, 16)), cols((PTS, 16))

    def edge_column(table):
        spread_out = jnp.zeros((PTS, 16), F32)
        for s in range(4):
            here = ((edge_row >> 4) == edge_col) & (((edge_row >> 2) & 3) == s)
            line = table[pl.ds(s, 1), :].astype(F32)
            spread_out = jnp.where(here, jnp.broadcast_to(line, (PTS, 16)), spread_out)
        return jnp.sum(spread_out, axis=1, keepdims=True).astype(I32)

    ne, nt = edge_column(nel), edge_column(ned)
    off = offset_of(ne >> 4, me, count)
    pe = (ne & 15) * 4 + nt
    off_f, pe_f = off.astype(F32), pe.astype(F32)
    off_row = jnp.sum(jnp.where(unit, off_f, 0.0), axis=0, keepdims=True)
    pe_row = jnp.sum(jnp.where(unit, pe_f, 0.0), axis=0, keepdims=True)
    peer = (off_row == off_f) & ((c & 3) == 0)
    rank_own = jnp.sum(jnp.where(peer & ((c >> 2) < (r >> 2)), 1.0, 0.0), axis=1, keepdims=True).astype(I32)
    rank_pe = jnp.sum(jnp.where(peer & (pe_row < pe_f), 1.0, 0.0), axis=1, keepdims=True).astype(I32)
    point = rows((PTS, 1)) & 3
    slot = jnp.where(off == 1, pe, jnp.where(off == 0, 64 + rank_pe, 80 + rank_pe))
    take = (cols((PTS, 384)) == slot * 4 + 3 - point).astype(F32).astype(BF16)
    place = jnp.where(off == 1, -1, jnp.where(off == 2, 0, 64) + rank_own * 4 + point)
    pack_t = (cols((PTS, 128)) == place).astype(F32)
    pack = pack_t.T.astype(BF16)
    spread_t = (same_elem & ((r & 15) == edge_point((c >> 2) & 3, c & 3))).astype(F32).astype(BF16)
    spread = (same_elem & ((c & 15) == edge_point((r >> 2) & 3, r & 3))).astype(F32).astype(BF16)
    a, b = (rows((PTS, 1)) >> 2) & 3, rows((PTS, 1)) & 3
    rim_a, rim_b = ((a == 0) | (a == 3)).astype(F32), ((b == 0) | (b == 3)).astype(F32)
    counts = 1.0 + rim_a + rim_b
    added = dot(spread_t, take)
    own_add = dot(added[:, :PTS].astype(BF16), spread)
    r_own = (jnp.where(unit, 1.0, 0.0) + own_add) / counts
    r_out = added[:, PTS:] / counts
    picked = dot(pack, spread)
    km = dot_split(picked, m)
    g = dot_split(r_own, m)
    for side, through in enumerate((dot_split(km[:64], r_out[:, :64]), dot_split(km[64:], r_out[:, 64:]))):
        hi, lo = split(through)
        vz_hi[side] = hi
        vz_lo[side] = lo
    lands = ((off != 1) & (c == pe * 4 + 3 - point)).astype(F32).astype(BF16)
    landed = dot(pack, lands).T.astype(BF16)
    r_nb = dot(spread_t, landed) / counts
    for side, back in enumerate((dot_split(r_nb[:, 64:], km[64:]), dot_split(r_nb[:, :64], km[:64]))):
        hi, lo = split(back)
        back_hi[side] = hi
        back_lo[side] = lo
    kmg = dot_split(km, g)
    fold = ((rows((PTS, 128)) & 15) == cols((PTS, 128))).astype(F32)
    cut = dot_split(km, fold)
    for side in range(2):
        km_cut[side] = cut[64 * side : 64 * side + 64]
        km_twice[side] = kmg[64 * side : 64 * side + 64]
    unfold = (rows((128, PTS)) == (cols((128, PTS)) & 15)).astype(F32).astype(BF16)
    place_pe = jnp.where(off == 1, -1, jnp.where(off == 2, 0, 64) + rank_pe * 4 + point)
    arrive = (cols((PTS, 128)) == place_pe).astype(F32).T.astype(BF16)
    facing = dot(dot(arrive, lands).astype(BF16), same_elem.astype(F32).astype(BF16))
    mine[1] = (facing[:64] > 0.5).astype(F32)
    mine[0] = (facing[64:] > 0.5).astype(F32)
    for side in range(2):
        hi, lo = split(
            jnp.concatenate(
                [km[64 * side : 64 * side + 64], kmg[64 * side : 64 * side + 64]], axis=0
            )
        )
        sm_hi[side] = hi
        sm_lo[side] = lo
    gr = dot_split(g, r_out)
    gg = dot_split(g, g)
    ext = -VISCOSITY * jnp.concatenate([gr[:, :64], r_out[:, :64], gr[:, 64:], r_out[:, 64:]], axis=1)
    hi, lo = split(ext)
    e_hi[...] = hi
    e_lo[...] = lo

    def meet(side):
        ex_w(side).wait_recv()
        ex_c(side).wait_recv()
        shift = jnp.where(side == 0, 32.0, 0.0)
        for k in range(LEV):
            hi, lo, code = tiled(wx_in.at[side], cd_in.at[side], k)
            match = code == (lane_elem + shift)
            n_hi = jnp.where(match, hi, 0.0).astype(BF16)
            n_lo = jnp.where(match, lo, 0.0).astype(BF16)
            nb_hi[k, side] = n_hi
            nb_lo[k, side] = n_lo
            hi, lo = split(own_t[k].reshape(PTS, Q))
            fix[k, side] = dot3(n_hi, n_lo, hi, lo)

    def matrix_in(side, part):
        ex_m(side, part).wait_recv()
        if part == 0:
            hi, lo = split(km_in[side])
            hi, lo = split((dot(hi, unfold) + dot(lo, unfold)) * mine[side])
        else:
            hi, lo = split(km_twice_in[side])
        sn_hi[side, part] = hi
        sn_lo[side, part] = lo

    def take(k, side):
        hi, lo = split(first[k])
        hi, lo = split(dot3(nb_hi[k, side], nb_lo[k, side], hi, lo))
        taken_hi[k, side] = hi
        taken_lo[k, side] = lo

    def correct_once(k, side):
        corr[k, side, pl.ds(0, 64)] = dot3(
            sn_hi[side, 0], sn_lo[side, 0], taken_hi[k, side], taken_lo[k, side]
        )

    def correct_twice(side):
        matrix_in(side, 1)
        for k in range(LEV):
            corr[k, side, pl.ds(64, 64)] = dot3(
                sn_hi[side, 1], sn_lo[side, 1], taken_hi[k, side], taken_lo[k, side]
            )

    def second_from(k, side, start):
        ex2(k, side).wait_recv()
        part = mix(k, 2 * side, f2[k, side].reshape(PTS, Q) + fix[k, side])
        here = base[k]
        hi, lo = split(here + part)
        terms = dot3(sm_hi[side], sm_lo[side], hi, lo)
        once[k, side] = terms[:64]
        twice_own[k, side] = terms[64:]
        ex_p(k, side).start()
        total[k] = (here if start else total[k]) + part

    def settle(k):
        hi, lo = split(total[k])
        total[k] = dot3(h_hi[...], h_lo[...], hi, lo)

    def relay(k, side):
        ex_p(k, side).wait_recv()
        whole = once_in[k, side] + corr[k, side, pl.ds(0, 64)]
        terms_in[k, side, pl.ds(0, 64)] = whole
        hi, lo = split(whole)
        twice[k, side] = twice_own[k, side] + dot3(vz_hi[side], vz_lo[side], hi, lo)
        ex_q(k, side).start()

    meet(twin)

    @pl.when(first_of_all)
    def _():
        send_tracers(True)
        send_tables()

    for k in range(LEV):
        ex1(k, twin).wait_recv()
        value = own[k] + mix(k, 2 * twin, f1[k, twin])
        partial[k, twin] = cube(value)
        ex2(k, twin).start()
        first[k] = value
    for part in range(2):
        for side in range(2):
            ex_m(side, part).start()

    for k in range(LEV):
        ex1(k, remote_side).wait_recv()
        part = mix(k, 2 * remote_side, f1[k, remote_side])
        partial[k, remote_side] = cube(own[k] + part)
        ex2(k, remote_side).start()
        value = first[k] + part
        first[k] = value
        base[k] = mix(k, 1, value) + src[k].reshape(PTS, Q)

        @pl.when(edge)
        def _():
            second_from(k, near, True)
            if k == 1:
                matrix_in(near, 0)
            if k >= 1:
                take(k - 1, near)
                correct_once(k - 1, near)

    @pl.when(edge)
    def _():
        take(LEV - 1, near)
        correct_once(LEV - 1, near)
        for k in range(LEV):
            relay(k, near)

    meet(remote_side)

    @pl.when(jnp.logical_not(edge))
    def _():
        for k in range(LEV):
            second_from(k, ahead, True)
        for k in range(LEV):
            second_from(k, 1 - ahead, False)
        for k in range(LEV):
            take(k, near)
            take(k, far)
        matrix_in(near, 0)
        for k in range(LEV):
            correct_once(k, near)
            relay(k, near)
    correct_twice(near)

    @pl.when(edge)
    def _():
        for k in range(LEV):
            second_from(k, far, False)
            take(k, far)

    matrix_in(far, 0)
    for k in range(LEV):
        correct_once(k, far)
    through = jnp.concatenate(
        [dot3(sn_hi[side, 0], sn_lo[side, 0], back_hi[side], back_lo[side]) for side in range(2)], axis=0
    )
    h = jnp.where(unit, 1.0, 0.0) - VISCOSITY * (gg + dot_split(r_out, through))
    hi, lo = split(h)
    h_hi[...] = hi
    h_lo[...] = lo

    for k in range(LEV):
        relay(k, far)
        if k % 2 == 0:
            settle(k // 2)
    for k in (LEV - 2, LEV - 1):
        settle(k)
    correct_twice(far)
    for k in range(LEV):
        wait_bytes(twice_in.at[k], recvq.at[k])
        for side in range(2):
            terms_in[k, side, pl.ds(64, 64)] = twice_in[k, side] + corr[k, side, pl.ds(64, 64)]
        hi, lo = split(terms_in[k].reshape(PTS, Q))
        outbuf[:, k] = cube(total[k] + dot3(e_hi[...], e_lo[...], hi, lo))

    for side in range(2):
        wait_bytes(span, sent.at[side])


def local(tracers, sources, weights, dep_owner, dep_slot, nbr_elem, nbr_edge, metric):
    count = lax.axis_size("elem")
    block = (LEV, 16, 16, Q)
    dma = pltpu.SemaphoreType.DMA
    vmem = pltpu.VMEM
    pairs = (LEV, 2, 16, 16, Q)
    flat = (LEV, PTS, Q)
    tall = (2, 128, PTS)
    slim = (LEV, 2, 64, Q)
    scratch = [
        vmem(block, F32), vmem(block, F32), vmem((16, LEV, PTS), F32), vmem((16, 128), F32),
        vmem((2, 16, 128), F32), vmem(dep_owner.shape, I32), vmem(dep_slot.shape, I32),
        vmem(nbr_elem.shape[::-1], I32), vmem(nbr_edge.shape[::-1], I32), vmem(metric.shape, F32),
        vmem(pairs, F32), vmem(flat, F32), vmem(pairs, F32), vmem(flat, F32),
        vmem(pairs, F32), vmem((LEV, 2, PTS, Q), F32), vmem(flat, F32), vmem(flat, F32),
        vmem((LEV, 3, PTS, PTS), BF16), vmem((LEV, 3, PTS, PTS), BF16),
        vmem((2, 16, LEV, PTS), F32), vmem((LEV, 2, PTS, PTS), BF16), vmem((LEV, 2, PTS, PTS), BF16),
        vmem((LEV, 2, PTS, Q), BF16), vmem((LEV, 2, PTS, Q), BF16), vmem((181, 16, 128), F32),
        vmem((2, 64, 128), F32), vmem((2, 64, 128), F32), vmem((2, 64, PTS), F32),
        vmem((2, 64, PTS), F32), vmem((2, 64, PTS), F32), vmem(tall, BF16), vmem(tall, BF16),
        vmem((2, 2, 64, PTS), BF16), vmem((2, 2, 64, PTS), BF16),
        vmem((LEV, 2, 128, Q), F32), vmem((2, 64, 64), BF16), vmem((2, 64, 64), BF16),
        vmem(slim, F32), vmem(slim, F32), vmem(slim, F32), vmem(slim, F32), vmem(slim, F32),
        vmem((LEV, 2, 128, Q), F32),
        vmem((PTS, PTS), BF16), vmem((PTS, PTS), BF16),
        vmem((PTS, PTS), BF16), vmem((PTS, PTS), BF16),
        vmem((2, PTS, PTS), BF16), vmem((2, PTS, PTS), BF16),
        dma((6,)), dma((1 + LEV,)),
        dma((2,)), dma((LEV, 2)), dma((LEV, 2)), dma((4, 2)), dma((LEV, 2)), dma((LEV,)),
    ]
    return pl.pallas_call(
        functools.partial(kernel, count),
        out_shape=pltpu.VMEM(tracers.shape, F32),
        in_specs=[pl.BlockSpec(memory_space=pl.ANY)] * 8,
        out_specs=pl.BlockSpec(memory_space=pltpu.VMEM),
        scratch_shapes=scratch,
        compiler_params=pltpu.CompilerParams(collective_id=0, has_side_effects=True),
        name="tracer_step",
    )(tracers, sources, weights, dep_owner, dep_slot, nbr_elem.T, nbr_edge.T, metric)


def solution(mesh):
    placed = (
        P("elem", None, None, None),
        P("elem", None, None, None),
        P("elem", None, None),
        P("elem", None, None),
        P("elem", None, None),
        P("elem", None),
        P("elem", None),
        P("elem", None, None),
    )
    return jax.shard_map(
        local, mesh=mesh, in_specs=placed, out_specs=P("elem", None, None, None), check_vma=False
    )
```

```python
import functools

import jax
import jax.numpy as jnp
import numpy as np
from jax import lax
from jax.experimental import pallas as pl
from jax.experimental.pallas import tpu as pltpu
from jax.sharding import PartitionSpec as P

VISCOSITY = 0.002
LEV = 4
PTS = 256
Q = 128
F32 = jnp.float32
BF16 = jnp.bfloat16
I32 = jnp.int32


def derivative_matrix():
    nodes = np.array([-1.0, -np.sqrt(0.2), np.sqrt(0.2), 1.0])
    count = nodes.shape[0]
    bary = np.array(
        [1.0 / np.prod([nodes[j] - nodes[m] for m in range(count) if m != j]) for j in range(count)]
    )
    derivative = np.zeros((count, count))
    for i in range(count):
        for j in range(count):
            if i != j:
                derivative[i, j] = bary[j] / bary[i] / (nodes[i] - nodes[j])
        derivative[i, i] = -np.sum(derivative[i])
    return derivative


def rows(shape):
    return lax.broadcasted_iota(I32, shape, 0)


def cols(shape):
    return lax.broadcasted_iota(I32, shape, 1)


def dot(a, b):
    return jnp.dot(a, b, preferred_element_type=F32)


def split(x):
    hi = x.astype(BF16)
    lo = (x - hi.astype(F32)).astype(BF16)
    return hi, lo


def dot3(a_hi, a_lo, b_hi, b_lo):
    n = b_hi.shape[1]
    both = dot(a_hi, jnp.concatenate([b_hi, b_lo], axis=1))
    return both[:, :n] + (both[:, n:] + dot(a_lo, b_hi))


def dot_split(a, b):
    return dot3(*split(a), *split(b))


def edge_point(s, k):
    return jnp.where(s == 0, 4 * k, jnp.where(s == 1, 12 + k, jnp.where(s == 2, 15 - 4 * k, 3 - k)))


def direction_table(shape, along_b):
    m, p = rows(shape) & 15, cols(shape) & 15
    if along_b:
        i, j, live = m & 3, p & 3, (m >> 2) == (p >> 2)
    else:
        i, j, live = m >> 2, p >> 2, (m & 3) == (p & 3)
    which = jnp.where(live, i * 4 + j, -1)
    table = derivative_matrix()
    value = jnp.zeros(shape, F32)
    for at in range(16):
        value = jnp.where(which == at, np.float32(table[at // 4, at % 4]), value)
    return value


def offset_of(owner, me, count):
    d = owner - me
    d = jnp.where(d > 1, d - count, d)
    d = jnp.where(d < -1, d + count, d)
    return d + 1


def kernel(
    count,
    tracers, sources, weights, dep_owner, dep_slot, nbr_elem, nbr_edge, metric,
    outbuf,
    own_t, src, wx, cd, cd_in, dow, dsl, nel, ned, met,
    f1, own, partial, first, f2, fix, base, total,
    w_hi, w_lo, wx_in, nb_hi, nb_lo, taken_hi, taken_lo, span,
    km_cut, km_in, km_twice, km_twice_in, mine, sm_hi, sm_lo, sn_hi, sn_lo,
    corr, vz_hi, vz_lo, once, twice_own, twice, once_in, twice_in, terms_in,
    h_hi, h_lo, e_hi, e_lo, back_hi, back_lo,
    loc, loc_t,
    sent, recv1, recv2, recvm, recvp, recvq,
):
    me = lax.axis_index("elem")
    place_in_row = lax.rem(me, 8)
    near = jnp.where(place_in_row < 4, 1, 0)
    far = 1 - near
    edge = (place_in_row == 0) | (place_in_row == 7)
    twin = jnp.where(lax.rem(me, 2) == 0, 1, 0)
    remote_side = 1 - twin
    middle = (place_in_row == 3) | (place_in_row == 4)
    ahead = jnp.where(middle, far, near)

    def beyond(side):
        return lax.rem(me + 1 - 2 * side + count, count)

    def remote(source, target, send_sem, recv_sem, side):
        return pltpu.make_async_remote_copy(
            src_ref=source,
            dst_ref=target,
            send_sem=send_sem,
            recv_sem=recv_sem,
            device_id=(beyond(side),),
            device_id_type=pl.DeviceIdType.MESH,
        )

    small = [
        pltpu.make_async_copy(a, b, loc.at[i])
        for i, (a, b) in enumerate(
            [
                (weights, wx),
                (dep_owner, dow),
                (dep_slot, dsl),
                (nbr_elem, nel),
                (nbr_edge, ned),
                (metric, met),
            ]
        )
    ]
    load_t = [pltpu.make_async_copy(tracers.at[:, k], own_t.at[k], loc_t.at[1 + k]) for k in range(LEV)]
    load_s = [pltpu.make_async_copy(sources.at[:, k], src.at[k], loc_t.at[0]) for k in range(LEV)]

    def wait_bytes(like, semaphore):
        pltpu.make_async_copy(like, like, semaphore).wait()

    def ex1(k, side):
        return remote(own_t.at[k], f1.at[k, side], sent.at[side], recv1.at[k, side], side)

    def ex2(k, side):
        return remote(partial.at[k, side], f2.at[k, side], sent.at[side], recv2.at[k, side], side)

    def ex_w(side):
        return remote(wx, wx_in.at[side], sent.at[side], recvm.at[0, side], side)

    def ex_c(side):
        return remote(cd, cd_in.at[side], sent.at[side], recvm.at[3, side], side)

    def ex_m(side, part):
        ends = ((km_cut, km_in), (km_twice, km_twice_in))[part]
        return remote(
            ends[0].at[side], ends[1].at[side], sent.at[side], recvm.at[1 + part, side], side
        )

    def ex_p(k, side):
        return remote(once.at[k, side], once_in.at[k, side], sent.at[side], recvp.at[k, side], side)

    def ex_q(k, side):
        return remote(twice.at[k, side], twice_in.at[k, side], sent.at[side], recvq.at[k], side)

    barrier = pltpu.get_barrier_semaphore()
    for side in range(2):
        pl.semaphore_signal(
            barrier, inc=1, device_id=(beyond(side),), device_id_type=pl.DeviceIdType.MESH
        )
    for c in load_t:
        c.start()
    for c in small:
        c.start()
    for c in load_s:
        c.start()

    def send_tracers(loaded):
        pl.semaphore_wait(barrier, 2)
        for k in range(LEV):
            if not loaded:
                load_t[k].wait()
            for side in range(2):
                ex1(k, side).start()

    def send_tables():
        for side in range(2):
            ex_w(side).start()
            ex_c(side).start()

    first_of_all = me == 0
    others = jnp.logical_not(first_of_all)

    @pl.when(others)
    def _():
        send_tracers(False)

    @pl.when(first_of_all)
    def _():
        for k in range(LEV):
            load_t[k].wait()

    for c in small:
        c.wait()
    cd[...] = jnp.zeros((16, 128), F32)
    for e in range(16):
        code = (offset_of(dow[e], me, count) * 16 + dsl[e]).astype(F32)
        for k in range(LEV):
            cd[pl.ds(e, 1), pl.ds(16 * k, 16)] = code[k : k + 1]
    pl.when(others)(send_tables)
    wait_bytes(src, loc_t.at[0])
    diagonal = (cols((16, PTS)) >> 4) == rows((16, PTS))
    eye16 = cols((16, 16)) == rows((16, 16))
    tile_j = ((rows((PTS, PTS)) & 15) == (cols((PTS, PTS)) & 15)).astype(F32).astype(BF16)
    lane_elem = (cols((1, PTS)) >> 4).astype(F32)

    def tiled(table, marks, k):
        his, los, codes = [], [], []
        for e in range(16):
            row = table[e, pl.ds(k, 1), :]
            hi = row.astype(BF16).astype(F32)
            his.append(jnp.where(diagonal, jnp.broadcast_to(hi, (16, PTS)), 0.0))
            los.append(jnp.where(diagonal, jnp.broadcast_to(row - hi, (16, PTS)), 0.0))
            code = marks[pl.ds(e, 1), pl.ds(16 * k, 16)]
            codes.append(jnp.where(eye16, jnp.broadcast_to(code, (16, 16)), 0.0))
        hi = dot(jnp.concatenate(his, axis=0).astype(BF16), tile_j)
        lo = dot(jnp.concatenate(los, axis=0).astype(BF16), tile_j)
        code = jnp.sum(jnp.concatenate(codes, axis=0), axis=1, keepdims=True)
        return hi, lo, code

    def mix(k, i, field):
        hi, lo = split(field.reshape(PTS, Q))
        return dot3(w_hi[k, i], w_lo[k, i], hi, lo)

    def cube(x):
        return x.reshape(16, 16, Q)

    for k in range(LEV):
        hi, lo, code = tiled(wx, cd, k)
        for i in range(3):
            match = code == (lane_elem + float(16 * i))
            w_hi[k, i] = jnp.where(match, hi, 0.0).astype(BF16)
            w_lo[k, i] = jnp.where(match, lo, 0.0).astype(BF16)
        own[k] = mix(k, 1, own_t[k]) + src[k].reshape(PTS, Q)

    square = (PTS, PTS)
    r, c = rows(square), cols(square)
    same_elem = (r >> 4) == (c >> 4)
    unit = r == c
    left_a, left_b = direction_table((16, 16), False), direction_table((16, 16), True)
    right_a, right_b = direction_table((16, PTS), False), direction_table((16, PTS), True)
    fa, fb = [], []
    for e in range(16):
        fa.append(left_a * jnp.broadcast_to(met[e, pl.ds(0, 1), :], (16, 16)))
        fb.append(left_b * jnp.broadcast_to(met[e, pl.ds(1, 1), :], (16, 16)))
    full = dot_split(jnp.concatenate(fa, axis=0), right_a) + dot_split(jnp.concatenate(fb, axis=0), right_b)
    m = jnp.where(same_elem, full, 0.0)

    edge_row, edge_col = rows((PTS, 16)), cols((PTS, 16))

    def edge_column(table):
        spread_out = jnp.zeros((PTS, 16), F32)
        for s in range(4):
            here = ((edge_row >> 4) == edge_col) & (((edge_row >> 2) & 3) == s)
            line = table[pl.ds(s, 1), :].astype(F32)
            spread_out = jnp.where(here, jnp.broadcast_to(line, (PTS, 16)), spread_out)
        return jnp.sum(spread_out, axis=1, keepdims=True).astype(I32)

    ne, nt = edge_column(nel), edge_column(ned)
    off = offset_of(ne >> 4, me, count)
    pe = (ne & 15) * 4 + nt
    off_f, pe_f = off.astype(F32), pe.astype(F32)
    off_row = jnp.sum(jnp.where(unit, off_f, 0.0), axis=0, keepdims=True)
    pe_row = jnp.sum(jnp.where(unit, pe_f, 0.0), axis=0, keepdims=True)
    peer = (off_row == off_f) & ((c & 3) == 0)
    rank_own = jnp.sum(jnp.where(peer & ((c >> 2) < (r >> 2)), 1.0, 0.0), axis=1, keepdims=True).astype(I32)
    rank_pe = jnp.sum(jnp.where(peer & (pe_row < pe_f), 1.0, 0.0), axis=1, keepdims=True).astype(I32)
    point = rows((PTS, 1)) & 3
    slot = jnp.where(off == 1, pe, jnp.where(off == 0, 64 + rank_pe, 80 + rank_pe))
    take = (cols((PTS, 384)) == slot * 4 + 3 - point).astype(F32).astype(BF16)
    place = jnp.where(off == 1, -1, jnp.where(off == 2, 0, 64) + rank_own * 4 + point)
    pack_t = (cols((PTS, 128)) == place).astype(F32)
    pack = pack_t.T.astype(BF16)
    spread_t = (same_elem & ((r & 15) == edge_point((c >> 2) & 3, c & 3))).astype(F32).astype(BF16)
    spread = (same_elem & ((c & 15) == edge_point((r >> 2) & 3, r & 3))).astype(F32).astype(BF16)
    a, b = (rows((PTS, 1)) >> 2) & 3, rows((PTS, 1)) & 3
    rim_a, rim_b = ((a == 0) | (a == 3)).astype(F32), ((b == 0) | (b == 3)).astype(F32)
    counts = 1.0 + rim_a + rim_b
    added = dot(spread_t, take)
    own_add = dot(added[:, :PTS].astype(BF16), spread)
    r_own = (jnp.where(unit, 1.0, 0.0) + own_add) / counts
    r_out = added[:, PTS:] / counts
    picked = dot(pack, spread)
    km = dot_split(picked, m)
    g = dot_split(r_own, m)
    for side, through in enumerate((dot_split(km[:64], r_out[:, :64]), dot_split(km[64:], r_out[:, 64:]))):
        hi, lo = split(through)
        vz_hi[side] = hi
        vz_lo[side] = lo
    lands = ((off != 1) & (c == pe * 4 + 3 - point)).astype(F32).astype(BF16)
    landed = dot(pack, lands).T.astype(BF16)
    r_nb = dot(spread_t, landed) / counts
    for side, back in enumerate((dot_split(r_nb[:, 64:], km[64:]), dot_split(r_nb[:, :64], km[:64]))):
        hi, lo = split(back)
        back_hi[side] = hi
        back_lo[side] = lo
    kmg = dot_split(km, g)
    fold = ((rows((PTS, 128)) & 15) == cols((PTS, 128))).astype(F32)
    cut = dot_split(km, fold)
    for side in range(2):
        km_cut[side] = cut[64 * side : 64 * side + 64]
        km_twice[side] = kmg[64 * side : 64 * side + 64]
    unfold = (rows((128, PTS)) == (cols((128, PTS)) & 15)).astype(F32).astype(BF16)
    place_pe = jnp.where(off == 1, -1, jnp.where(off == 2, 0, 64) + rank_pe * 4 + point)
    arrive = (cols((PTS, 128)) == place_pe).astype(F32).T.astype(BF16)
    facing = dot(dot(arrive, lands).astype(BF16), same_elem.astype(F32).astype(BF16))
    mine[1] = (facing[:64] > 0.5).astype(F32)
    mine[0] = (facing[64:] > 0.5).astype(F32)
    for side in range(2):
        hi, lo = split(
            jnp.concatenate(
                [km[64 * side : 64 * side + 64], kmg[64 * side : 64 * side + 64]], axis=0
            )
        )
        sm_hi[side] = hi
        sm_lo[side] = lo
    gr = dot_split(g, r_out)
    gg = dot_split(g, g)
    ext = -VISCOSITY * jnp.concatenate([gr[:, :64], r_out[:, :64], gr[:, 64:], r_out[:, 64:]], axis=1)
    hi, lo = split(ext)
    e_hi[...] = hi
    e_lo[...] = lo

    def meet(side):
        ex_w(side).wait_recv()
        ex_c(side).wait_recv()
        shift = jnp.where(side == 0, 32.0, 0.0)
        for k in range(LEV):
            hi, lo, code = tiled(wx_in.at[side], cd_in.at[side], k)
            match = code == (lane_elem + shift)
            n_hi = jnp.where(match, hi, 0.0).astype(BF16)
            n_lo = jnp.where(match, lo, 0.0).astype(BF16)
            nb_hi[k, side] = n_hi
            nb_lo[k, side] = n_lo
            hi, lo = split(own_t[k].reshape(PTS, Q))
            fix[k, side] = dot3(n_hi, n_lo, hi, lo)

    def matrix_in(side, part):
        ex_m(side, part).wait_recv()
        if part == 0:
            hi, lo = split(km_in[side])
            hi, lo = split((dot(hi, unfold) + dot(lo, unfold)) * mine[side])
        else:
            hi, lo = split(km_twice_in[side])
        sn_hi[side, part] = hi
        sn_lo[side, part] = lo

    def take(k, side):
        hi, lo = split(first[k])
        hi, lo = split(dot3(nb_hi[k, side], nb_lo[k, side], hi, lo))
        taken_hi[k, side] = hi
        taken_lo[k, side] = lo

    def correct_once(k, side):
        corr[k, side, pl.ds(0, 64)] = dot3(
            sn_hi[side, 0], sn_lo[side, 0], taken_hi[k, side], taken_lo[k, side]
        )

    def correct_twice(side):
        matrix_in(side, 1)
        for k in range(LEV):
            corr[k, side, pl.ds(64, 64)] = dot3(
                sn_hi[side, 1], sn_lo[side, 1], taken_hi[k, side], taken_lo[k, side]
            )

    def second_from(k, side, start):
        ex2(k, side).wait_recv()
        part = mix(k, 2 * side, f2[k, side].reshape(PTS, Q) + fix[k, side])
        here = base[k]
        hi, lo = split(here + part)
        terms = dot3(sm_hi[side], sm_lo[side], hi, lo)
        once[k, side] = terms[:64]
        twice_own[k, side] = terms[64:]
        ex_p(k, side).start()
        total[k] = (here if start else total[k]) + part

    def settle(k):
        hi, lo = split(total[k])
        total[k] = dot3(h_hi[...], h_lo[...], hi, lo)

    def relay(k, side):
        ex_p(k, side).wait_recv()
        whole = once_in[k, side] + corr[k, side, pl.ds(0, 64)]
        terms_in[k, side, pl.ds(0, 64)] = whole
        hi, lo = split(whole)
        twice[k, side] = twice_own[k, side] + dot3(vz_hi[side], vz_lo[side], hi, lo)
        ex_q(k, side).start()

    meet(twin)

    @pl.when(first_of_all)
    def _():
        send_tracers(True)
        send_tables()

    for k in range(LEV):
        ex1(k, twin).wait_recv()
        value = own[k] + mix(k, 2 * twin, f1[k, twin])
        partial[k, twin] = cube(value)
        ex2(k, twin).start()
        first[k] = value
    for side in range(2):
        ex_m(side, 0).start()

    @pl.when(jnp.logical_not(edge))
    def _():
        for side in range(2):
            ex_m(side, 1).start()


    for k in range(LEV):
        ex1(k, remote_side).wait_recv()
        part = mix(k, 2 * remote_side, f1[k, remote_side])
        partial[k, remote_side] = cube(own[k] + part)
        ex2(k, remote_side).start()
        value = first[k] + part
        first[k] = value
        base[k] = mix(k, 1, value) + src[k].reshape(PTS, Q)

        @pl.when(edge)
        def _():
            second_from(k, near, True)
            if k == 1:
                matrix_in(near, 0)
            if k >= 1:
                take(k - 1, near)
                correct_once(k - 1, near)

    @pl.when(edge)
    def _():
        for side in range(2):
            ex_m(side, 1).start()
        take(LEV - 1, near)
        correct_once(LEV - 1, near)
        for k in range(LEV):
            relay(k, near)

    meet(remote_side)

    @pl.when(jnp.logical_not(edge))
    def _():
        for k in range(LEV):
            second_from(k, ahead, True)
        for k in range(LEV):
            second_from(k, 1 - ahead, False)
        for k in range(LEV):
            take(k, near)
            take(k, far)
        matrix_in(near, 0)
        for k in range(LEV):
            correct_once(k, near)
            relay(k, near)
    correct_twice(near)

    @pl.when(edge)
    def _():
        for k in range(LEV):
            second_from(k, far, False)
            take(k, far)

    matrix_in(far, 0)
    for k in range(LEV):
        correct_once(k, far)
    through = jnp.concatenate(
        [dot3(sn_hi[side, 0], sn_lo[side, 0], back_hi[side], back_lo[side]) for side in range(2)], axis=0
    )
    h = jnp.where(unit, 1.0, 0.0) - VISCOSITY * (gg + dot_split(r_out, through))
    hi, lo = split(h)
    h_hi[...] = hi
    h_lo[...] = lo

    for k in range(LEV):
        relay(k, far)
        if k % 2 == 0:
            settle(k // 2)
    for k in (LEV - 2, LEV - 1):
        settle(k)
    correct_twice(far)
    for k in range(LEV):
        wait_bytes(twice_in.at[k], recvq.at[k])
        for side in range(2):
            terms_in[k, side, pl.ds(64, 64)] = twice_in[k, side] + corr[k, side, pl.ds(64, 64)]
        hi, lo = split(terms_in[k].reshape(PTS, Q))
        outbuf[:, k] = cube(total[k] + dot3(e_hi[...], e_lo[...], hi, lo))

    for side in range(2):
        wait_bytes(span, sent.at[side])


def local(tracers, sources, weights, dep_owner, dep_slot, nbr_elem, nbr_edge, metric):
    count = lax.axis_size("elem")
    block = (LEV, 16, 16, Q)
    dma = pltpu.SemaphoreType.DMA
    vmem = pltpu.VMEM
    pairs = (LEV, 2, 16, 16, Q)
    flat = (LEV, PTS, Q)
    tall = (2, 128, PTS)
    slim = (LEV, 2, 64, Q)
    scratch = [
        vmem(block, F32), vmem(block, F32), vmem((16, LEV, PTS), F32), vmem((16, 128), F32),
        vmem((2, 16, 128), F32), vmem(dep_owner.shape, I32), vmem(dep_slot.shape, I32),
        vmem(nbr_elem.shape[::-1], I32), vmem(nbr_edge.shape[::-1], I32), vmem(metric.shape, F32),
        vmem(pairs, F32), vmem(flat, F32), vmem(pairs, F32), vmem(flat, F32),
        vmem(pairs, F32), vmem((LEV, 2, PTS, Q), F32), vmem(flat, F32), vmem(flat, F32),
        vmem((LEV, 3, PTS, PTS), BF16), vmem((LEV, 3, PTS, PTS), BF16),
        vmem((2, 16, LEV, PTS), F32), vmem((LEV, 2, PTS, PTS), BF16), vmem((LEV, 2, PTS, PTS), BF16),
        vmem((LEV, 2, PTS, Q), BF16), vmem((LEV, 2, PTS, Q), BF16), vmem((181, 16, 128), F32),
        vmem((2, 64, 128), F32), vmem((2, 64, 128), F32), vmem((2, 64, PTS), F32),
        vmem((2, 64, PTS), F32), vmem((2, 64, PTS), F32), vmem(tall, BF16), vmem(tall, BF16),
        vmem((2, 2, 64, PTS), BF16), vmem((2, 2, 64, PTS), BF16),
        vmem((LEV, 2, 128, Q), F32), vmem((2, 64, 64), BF16), vmem((2, 64, 64), BF16),
        vmem(slim, F32), vmem(slim, F32), vmem(slim, F32), vmem(slim, F32), vmem(slim, F32),
        vmem((LEV, 2, 128, Q), F32),
        vmem((PTS, PTS), BF16), vmem((PTS, PTS), BF16),
        vmem((PTS, PTS), BF16), vmem((PTS, PTS), BF16),
        vmem((2, PTS, PTS), BF16), vmem((2, PTS, PTS), BF16),
        dma((6,)), dma((1 + LEV,)),
        dma((2,)), dma((LEV, 2)), dma((LEV, 2)), dma((4, 2)), dma((LEV, 2)), dma((LEV,)),
    ]
    return pl.pallas_call(
        functools.partial(kernel, count),
        out_shape=pltpu.VMEM(tracers.shape, F32),
        in_specs=[pl.BlockSpec(memory_space=pl.ANY)] * 8,
        out_specs=pl.BlockSpec(memory_space=pltpu.VMEM),
        scratch_shapes=scratch,
        compiler_params=pltpu.CompilerParams(collective_id=0, has_side_effects=True),
        name="tracer_step",
    )(tracers, sources, weights, dep_owner, dep_slot, nbr_elem.T, nbr_edge.T, metric)


def solution(mesh):
    placed = (
        P("elem", None, None, None),
        P("elem", None, None, None),
        P("elem", None, None),
        P("elem", None, None),
        P("elem", None, None),
        P("elem", None),
        P("elem", None),
        P("elem", None, None),
    )
    return jax.shard_map(
        local, mesh=mesh, in_specs=placed, out_specs=P("elem", None, None, None), check_vma=False
    )
```
